128 devices in a mesh: gx: 4 (over y), gy: 8 (over x, core), gz: 4 (over z).
Axes of the slice: x: 4, y: 4, z: 4, core: 2. Of those that a mesh axis runs over, the one named last changes fastest.
Arguments:
- rhs: float32 [8, 64, 256, 512], P(None, 'gx', 'gy', 'gz'), may hold values from -8 to 8
- stencil: float32 [14, 64, 256, 512], P(None, 'gx', 'gy', 'gz'), may hold values from 0.02 to 1
Outputs:
- solution: float32 [8, 64, 256, 512], P(None, 'gx', 'gy', 'gz')
- residual: float32 [8, 64, 256, 512], P(None, 'gx', 'gy', 'gz')
The draws below stay inside these ranges and needn't reach their ends.
All inputs are finite; a program needn't handle non-finite values.
Results may differ from the reference program's by a relative error of at most 0.00029.
Values sent between devices are 32-bit elements; how exact they have to be, the bound alone decides.
No kernel may reach another device: no remote copies, remote signals or barrier semaphores. Data moves between devices by JAX's collectives and lax.ppermute only.
A program may use at most 128 MiB of HBM per device.

```python
import math
import jax
import jax.numpy as jnp
from jax import lax

NRHS = 8
ITERS = 2
NX = 64
NY = 256
NZ = 512


def block_levels(own_key, dims, shards, low, high):
    level = 1.0
    for dim, blocks in shards:
        steps = jax.random.uniform(jax.random.fold_in(jax.random.fold_in(own_key, 6), dim), (blocks,), jnp.float32, low / len(shards), high / len(shards))
        level = level * jnp.repeat(jnp.exp(steps), dims[dim] // blocks).reshape((-1,) + (1,) * (len(dims) - 1 - dim))
    return level


def bell_draw(rng, shape, scale, bound, split=(), dtype=jnp.bfloat16):
    level = block_levels(rng, shape, split, -0.22, 0.18) if split else 1.0
    values = jax.random.normal(rng, shape, jnp.float32) * scale * level
    return jnp.minimum(jnp.maximum(values, -bound), bound).astype(dtype)


def setup_inputs(seed: int = 0) -> dict:
    seeds = jax.random.split(jax.random.key(seed), 3)
    return {
        "rhs": bell_draw(seeds[0], (NRHS, NX, NY, NZ), 1.0, 8.0, ((1, 4), (2, 8), (3, 4)), jnp.float32),
        "stencil": jnp.clip(jnp.exp(math.log(1.0) - 3.912023 * jax.random.uniform(seeds[1], (14, NX, NY, NZ), jnp.float32) ** block_levels(seeds[1], (14, NX, NY, NZ), ((1, 4), (2, 8), (3, 4)), -0.2, 0.2)), 0.02, 1.0),
    }


FORWARD = [(a, b, c) for a in (-1, 0, 1) for b in (-1, 0, 1) for c in (-1, 0, 1) if (a, b, c) > (0, 0, 0)]

def window(array, margin, depth, offset):
    result = array
    for place in range(3):
        dim = array.ndim - 3 + place
        inner = array.shape[dim] - 2 * margin
        begin = margin - depth + offset[place]
        result = lax.slice_in_dim(result, begin, begin + inner + 2 * depth, axis=dim)
    return result

def diagonal_field(padded, margin, depth):
    total = window(padded[0], margin, depth, (0, 0, 0))
    total = total + jnp.sum(window(padded[1:], margin, depth, (0, 0, 0)), axis=0)
    for index, offset in enumerate(FORWARD):
        back = (-offset[0], -offset[1], -offset[2])
        total = total + window(padded[index + 1], margin, depth, back)
    return total

def operate(field, fmargin, padded, smargin, diag, depth):
    result = diag[None] * window(field, fmargin, depth, (0, 0, 0))
    for index, offset in enumerate(FORWARD):
        back = (-offset[0], -offset[1], -offset[2])
        ahead_w = window(padded[index + 1], smargin, depth, (0, 0, 0))
        behind_w = window(padded[index + 1], smargin, depth, back)
        result = result - ahead_w[None] * window(field, fmargin, depth, offset)
        result = result - behind_w[None] * window(field, fmargin, depth, back)
    return result

def gram(left, right):
    flat_l = left.reshape(left.shape[0], -1)
    flat_r = right.reshape(right.shape[0], -1)
    return lax.dot_general(flat_l.astype(jnp.float32), flat_r.astype(jnp.float32), (((1,), (1,)), ((), ())), precision=lax.Precision.HIGHEST, preferred_element_type=jnp.float32)

def combine(coef, field):
    return jnp.einsum('ij,ixyz->jxyz', coef, field, precision=lax.Precision.HIGHEST)

def solve_spd(matrix, right):
    factor = jnp.linalg.cholesky(matrix)
    return jax.scipy.linalg.cho_solve((factor, True), right)

def reference(rhs, stencil):
    padded = jnp.pad(stencil, ((0, 0), (1, 1), (1, 1), (1, 1)))
    diag = diagonal_field(padded, 1, 0)
    solution = jnp.zeros_like(rhs)
    residual = rhs
    direction = rhs
    norm_now = gram(residual, residual)
    for step in range(ITERS):
        field = jnp.pad(direction, ((0, 0), (1, 1), (1, 1), (1, 1)))
        image = operate(field, 1, padded, 1, diag, 0)
        alpha = solve_spd(gram(direction, image), norm_now)
        solution = solution + combine(alpha, direction)
        residual = residual - combine(alpha, image)
        if step + 1 < ITERS:
            norm_next = gram(residual, residual)
            beta = solve_spd(norm_now, norm_next)
            direction = residual + combine(beta, direction)
            norm_now = norm_next
    return (solution, residual)
```

```python
import jax
import jax.numpy as jnp
from jax import lax
from jax.experimental import pallas as pl
from jax.experimental.pallas import tpu as pltpu
from jax.sharding import PartitionSpec as P

F32 = jnp.float32
X, Y, Z, F = 16, 32, 128, 8
FORWARD = [
    (a, b, c) for a in (-1, 0, 1) for b in (-1, 0, 1) for c in (-1, 0, 1) if (a, b, c) > (0, 0, 0)
]
OFF = {k + 1: o for k, o in enumerate(FORWARD)}
ZPLUS = [k for k in OFF if OFF[k][2] == 1]
ZMINUS = [k for k in OFF if OFF[k][2] == -1]
YPLUS = [k for k in OFF if OFF[k][1] == 1]
YMINUS = [k for k in OFF if OFF[k][1] == -1]
XPLUS = [k for k in OFF if OFF[k][0] == 1]
ZSHIFTED = ZPLUS + ZMINUS
WZ_AT = {k: i for i, k in enumerate(ZSHIFTED)}
GROUPS = ((0, 1), (1, -1), (1, 0), (1, 1))
SHIFT_AT = {0: 0, -1: 1, 1: 2}

VSPEC = pl.BlockSpec(memory_space=pltpu.VMEM)
HSPEC = pl.BlockSpec(memory_space=pl.ANY)
MIB = 1024 * 1024


def call(body, name, ins, outs, aliases=None, scratch=(), out_specs=None, limit=8):
    return pl.pallas_call(
        body,
        name=name,
        out_shape=[jax.ShapeDtypeStruct(s, F32) for s in outs],
        in_specs=[VSPEC] * len(ins),
        out_specs=out_specs or [VSPEC] * len(outs),
        input_output_aliases=aliases or {},
        scratch_shapes=list(scratch),
        compiler_params=pltpu.CompilerParams(vmem_limit_bytes=limit * MIB),
    )(*ins)


def lanes():
    return lax.broadcasted_iota(jnp.int32, (8, 128), 1)


def rows():
    return lax.broadcasted_iota(jnp.int32, (8, 128), 0)


def roll(v, shift):
    shift %= 128
    return pltpu.roll(v, shift, axis=1) if shift else v


def put_first(value, source, lane):
    return jnp.where(lanes() == 0, roll(source, -lane), roll(value, 1))


def put_last(value, source, lane):
    return jnp.where(lanes() == 127, roll(source, 127 - lane), roll(value, 127))


def spot(x, y):
    return (x % 4) * 32 + y


def pack_columns(field, high_ref, low_ref, base=0):
    def group(g, carry):
        high = jnp.zeros((8, 128), F32)
        low = jnp.zeros((8, 128), F32)
        for xx in range(4):
            for y in range(Y):
                v = field[4 * g + xx, y]
                at = spot(xx, y)
                here = lanes() == at
                high = jnp.where(here, roll(v, at - 127), high)
                low = jnp.where(here, roll(v, at), low)
        high_ref[base + g] = high
        low_ref[base + g] = low
        return carry

    lax.fori_loop(0, 4, group, 0)


def start_kernel(rhs, st, vi, zp, zm):
    def turn(x, carry):
        for yb in range(4):
            vi[x, pl.ds(8 * yb, 8)] = jnp.swapaxes(rhs[:, x, pl.ds(8 * yb, 8), :], 0, 1)
        return carry

    lax.fori_loop(0, X, turn, 0)
    pack_columns(vi, zp, zm)
    for ref, keys, edge in ((zp, ZPLUS, 127), (zm, ZMINUS, 0)):
        for j, k in enumerate(keys):
            out = jnp.zeros((8, 128), F32)
            for x in range(X):
                for yb in range(4):
                    at = 4 * x + yb
                    w = st[k, x, pl.ds(8 * yb, 8), :]
                    out = jnp.where(lanes() == at, roll(w, at - edge), out)
            ref[4 + j] = out


def shift_fields(vi, rl, rr, vm, vp):
    def group(g, carry):
        left = rl[g]
        right = rr[g]
        for xx in range(4):
            for y in range(Y):
                v = vi[4 * g + xx, y]
                at = spot(xx, y)
                vm[4 * g + xx, y] = put_first(v, left, at)
                vp[4 * g + xx, y] = put_last(v, right, at)
        return carry

    lax.fori_loop(0, 4, group, 0)


def edge_rows(vi, rl, rr, yp, ym):
    for x in range(X):
        yp[x] = vi[x, Y - 1]
        ym[x] = vi[x, 0]
    for g in range(4):
        yp[16 + g] = rl[g]
        yp[20 + g] = rr[g]
        ym[16 + g] = rl[g]
        ym[20 + g] = rr[g]


def behind_row(st, wz, k, x, y):
    if k in WZ_AT:
        return wz[WZ_AT[k], x, pl.ds(y, 1), :]
    return st[k, x, pl.ds(y, 1), :]


def second_kernel(vi, st, rl, rr, vm, vp, wz, sums, yp, ym):
    shift_fields(vi, rl, rr, vm, vp)
    for keys, source, put in ((ZPLUS, rl, put_first), (ZMINUS, rr, put_last)):
        for j, k in enumerate(keys):
            column = source[4 + j]
            for x in range(X):
                for yb in range(4):
                    w = st[k, x, pl.ds(8 * yb, 8), :]
                    wz[WZ_AT[k], x, pl.ds(8 * yb, 8), :] = put(w, column, 4 * x + yb)

    def behind(k, x, yb):
        if k in WZ_AT:
            return wz[WZ_AT[k], x, pl.ds(8 * yb, 8), :]
        return st[k, x, pl.ds(8 * yb, 8), :]

    def add_up(x, carry):
        for yb in range(4):
            total = st[0, x, pl.ds(8 * yb, 8), :]
            for k in OFF:
                total = total + st[k, x, pl.ds(8 * yb, 8), :]
            sums[4, x, pl.ds(8 * yb, 8), :] = total + behind(1, x, yb)
            for i, (a, b) in enumerate(GROUPS):
                keys = [k for k in OFF if OFF[k][:2] == (a, b)]
                sums[i, x, pl.ds(8 * yb, 8), :] = (
                    behind(keys[0], x, yb) + behind(keys[1], x, yb) + behind(keys[2], x, yb)
                )
        return carry

    lax.fori_loop(0, X, add_up, 0)
    edge_rows(vi, rl, rr, yp, ym)
    for ref, keys, y in ((yp, YPLUS, Y - 1), (ym, YMINUS, 0)):
        for j, k in enumerate(keys):
            for x in range(X):
                r = 16 * j + x
                ref[24 + r // 8, pl.ds(r % 8, 1), :] = behind_row(st, wz, k, x, y)


def second_again_kernel(vi, rl, rr, vm, vp, yp, ym):
    shift_fields(vi, rl, rr, vm, vp)
    edge_rows(vi, rl, rr, yp, ym)


def wide(row):
    return jnp.broadcast_to(row, (8, 128))


def plane(x, first, last, fields, st, wz, acc_ref, at, diag_of):
    cache = {}

    def v(s, dx, y):
        key = (s, dx, y)
        if key not in cache:
            cache[key] = fields[SHIFT_AT[s]][x + dx, y]
        return cache[key]

    coef = {}

    def ahead(k, y):
        if OFF[k][2] == 0:
            if (k, 0, y) not in coef:
                coef[k, 0, y] = wide(st[k, x, pl.ds(y, 1), :])
            return coef[k, 0, y]
        return wide(st[k, x, pl.ds(y, 1), :])

    def behind(k, a, y):
        if k not in WZ_AT:
            if (k, a, y) not in coef:
                coef[k, a, y] = wide(st[k, x - a, pl.ds(y, 1), :])
            return coef[k, a, y]
        return wide(wz[WZ_AT[k], x - a, pl.ds(y, 1), :])

    for y in range(Y):
        parts = [None, None]
        n = 0
        for k, (a, b, c) in OFF.items():
            if 0 <= y + b < Y and not (a == 1 and last):
                term = ahead(k, y) * v(c, a, y + b)
                parts[n % 2] = term if parts[n % 2] is None else parts[n % 2] + term
                n += 1
            if 0 <= y - b < Y and not (a == 1 and first):
                term = behind(k, a, y - b) * v(-c, -a, y - b)
                parts[n % 2] = term if parts[n % 2] is None else parts[n % 2] + term
                n += 1
        acc_ref[at, y] = wide(diag_of(x, y, first)) * v(0, 0, y) - (parts[0] + parts[1])


def interior(fields, st, wz, acc_ref, lo, hi, diag_of):
    begin, end = lo, hi
    if lo == 0:
        plane(0, True, False, fields, st, wz, acc_ref, 0, diag_of)
        begin = 1
    if hi == X:
        end = hi - 1

    def step(x, carry):
        plane(x, False, False, fields, st, wz, acc_ref, x - lo, diag_of)
        return carry

    lax.fori_loop(begin, end, step, 0)
    if hi == X:
        plane(X - 1, False, True, fields, st, wz, acc_ref, X - 1 - lo, diag_of)


def inner_kernel(lo, hi):
    def body(vi, vm, vp, st, wz, sums, acc, diag):
        def diag_of(x, y, first):
            total = sums[4, x, pl.ds(y, 1), :]
            if y > 0:
                total = total + sums[0, x, pl.ds(y - 1, 1), :]
            if not first:
                total = total + sums[2, x - 1, pl.ds(y, 1), :]
                if y > 0:
                    total = total + sums[3, x - 1, pl.ds(y - 1, 1), :]
                if y < Y - 1:
                    total = total + sums[1, x - 1, pl.ds(y + 1, 1), :]
            diag[x - lo, pl.ds(y, 1), :] = total
            return total

        interior((vi, vm, vp), st, wz, acc, lo, hi, diag_of)

    return body


def inner_again_kernel(lo, hi):
    def body(vi, vm, vp, st, wz, diag_lo, diag_hi, acc):
        diag = diag_lo if lo == 0 else diag_hi

        def diag_of(x, y, first):
            return diag[x - lo, pl.ds(y, 1), :]

        interior((vi, vm, vp), st, wz, acc, lo, hi, diag_of)

    return body


def ring_row(ref, keys, k, x):
    r = 16 * keys.index(k) + x
    return ref[24 + r // 8, pl.ds(r % 8, 1), :]


def third_kernel(with_diag):
    def body(*refs):
        if with_diag:
            vi, vm, vp, st, wz, rl, rr, qm, qp, sums, ring, xm, xp = refs
            qmw, qpw = qm, qp
        else:
            vi, vm, vp, st, wz, rl, rr, qm, qp, qmw, qpw, ring, xm, xp = refs
        for side, q, y in ((0, qm, Y - 1), (1, qp, 0)):
            for x in range(X):
                v = q[x]
                ring[side, 0, x] = v
                ring[side, 1, x] = put_first(v, q[16 + x // 4], spot(x, y))
                ring[side, 2, x] = put_last(v, q[20 + x // 4], spot(x, y))
        xm[0] = qm[0]
        for y in range(Y):
            xm[1 + y] = vi[0, y]
        xm[Y + 1] = qp[0]
        for i, tile in enumerate((rl[0], rr[0], qm[16], qm[20], qp[16], qp[20])):
            xm[Y + 2 + i] = tile
        last = X - 1
        for y in range(Y):
            total = None
            for k in XPLUS:
                _, b, c = OFF[k]
                s = SHIFT_AT[-c]
                if y - b < 0:
                    term = wide(ring_row(qmw, YPLUS, k, last)) * ring[0, s, last]
                elif y - b >= Y:
                    term = wide(ring_row(qpw, YMINUS, k, last)) * ring[1, s, last]
                else:
                    term = wide(behind_row(st, wz, k, last, y - b)) * (vi, vm, vp)[s][last, y - b]
                total = term if total is None else total + term
            xp[y] = total
            if with_diag:
                row = sums[2, last, pl.ds(y, 1), :]
                if y > 0:
                    row = row + sums[3, last, pl.ds(y - 1, 1), :]
                else:
                    for k in (11, 12, 13):
                        row = row + ring_row(qmw, YPLUS, k, last)
                if y < Y - 1:
                    row = row + sums[1, last, pl.ds(y + 1, 1), :]
                else:
                    for k in (5, 6, 7):
                        row = row + ring_row(qpw, YMINUS, k, last)
                xp[Y + y // 8, pl.ds(y % 8, 1), :] = row

    return body


def far_plane(tp):
    far = {}
    for y in range(-1, Y + 1):
        v = tp[y + 1]
        base, lane = (Y + 2, y) if 0 <= y < Y else ((Y + 4, Y - 1) if y < 0 else (Y + 6, 0))
        far[0, y] = v
        far[-1, y] = put_first(v, tp[base], lane)
        far[1, y] = put_last(v, tp[base + 1], lane)
    return far


def finish_edges(acc_of, acc_set, st, ring, qmw, qpw, tp, tm, extra):
    last = X - 1
    far = {}

    def far_at(s, y):
        if (s, y) not in far:
            v = tp[y + 1]
            base, lane = (Y + 2, y) if 0 <= y < Y else ((Y + 4, Y - 1) if y < 0 else (Y + 6, 0))
            if s == 0:
                far[s, y] = v
            elif s < 0:
                far[s, y] = put_first(v, tp[base], lane)
            else:
                far[s, y] = put_last(v, tp[base + 1], lane)
        return far[s, y]

    for x in range(X):
        for y in range(Y) if x in (0, last) else (0, Y - 1):
            total = None
            for k, (a, b, c) in OFF.items():
                terms = []
                if x + a == X:
                    terms.append(wide(st[k, x, pl.ds(y, 1), :]) * far_at(c, y + b))
                elif y + b < 0:
                    terms.append(wide(st[k, x, pl.ds(y, 1), :]) * ring[0, SHIFT_AT[c], x + a])
                elif y + b >= Y:
                    terms.append(wide(st[k, x, pl.ds(y, 1), :]) * ring[1, SHIFT_AT[c], x + a])
                if x - a >= 0:
                    if y - b < 0:
                        terms.append(
                            wide(ring_row(qmw, YPLUS, k, x - a)) * ring[0, SHIFT_AT[-c], x - a]
                        )
                    elif y - b >= Y:
                        terms.append(
                            wide(ring_row(qpw, YMINUS, k, x - a)) * ring[1, SHIFT_AT[-c], x - a]
                        )
                for term in terms:
                    total = term if total is None else total + term
            if x == 0:
                total = tm[y] if total is None else total + tm[y]
            value = acc_of(x, y) - total
            if extra is not None:
                fix = extra(x, y)
                if fix is not None:
                    value = value + fix
            acc_set(x, y, value)


HALF = X // 2


class Halves:
    def __init__(self, lo, hi):
        self.lo, self.hi = lo, hi

    def __getitem__(self, index):
        x, y = index
        return self.lo[x, y] if x < HALF else self.hi[x - HALF, y]


def join_kernel(with_diag):
    def body(*refs):
        if with_diag:
            acc_lo, acc_hi, dg_lo, dg_hi, vi, st, ring, qm, qp, tp, tm, out, dlo, dhi, zp, zm = refs

            def fix(x, y):
                row = None
                if y == 0:
                    for k in (2, 3, 4):
                        r = ring_row(qm, YPLUS, k, x)
                        row = r if row is None else row + r
                    if x > 0:
                        for k in (11, 12, 13):
                            row = row + ring_row(qm, YPLUS, k, x - 1)
                if y == Y - 1 and x > 0:
                    for k in (5, 6, 7):
                        r = ring_row(qp, YMINUS, k, x - 1)
                        row = r if row is None else row + r
                if x == 0:
                    r = tm[Y + y // 8, pl.ds(y % 8, 1), :]
                    row = r if row is None else row + r
                if row is None:
                    return None
                d = dlo if x < HALF else dhi
                d[x % HALF, pl.ds(y, 1), :] = d[x % HALF, pl.ds(y, 1), :] + row
                return wide(row) * vi[x, y]

            dlo[...] = dg_lo[...]
            dhi[...] = dg_hi[...]
        else:
            acc_lo, acc_hi, st, ring, qm, qp, tp, tm, out = refs
            fix = None

        def copy_lo(x, carry):
            out[x] = acc_lo[x]
            out[x + HALF] = acc_hi[x]
            return carry

        lax.fori_loop(0, HALF, copy_lo, 0)

        def acc_set(x, y, value):
            out[x, y] = value

        finish_edges(Halves(acc_lo, acc_hi).__getitem__ and (lambda x, y: Halves(acc_lo, acc_hi)[x, y]),
                     acc_set, st, ring, qm, qp, tp, tm, fix)
        if with_diag:
            pack_columns(out, zp, zm)

    return body


def turn_slow(v, s):
    return pltpu.roll(v, s, axis=0) if s else v


def lane_sum(v):
    return jnp.broadcast_to(jnp.sum(v, axis=1, keepdims=True), (8, 128))


def diagonals(pairs_of, count):
    zero = tuple(jnp.zeros((8, 128), F32) for _ in range(count))

    def step(i, carry):
        carry = list(carry)
        for j in range(4):
            for n, term in enumerate(pairs_of(i // 8, (i % 8) * 4 + j)):
                carry[n] = carry[n] + term
        return tuple(carry)

    return lax.fori_loop(0, X * Y // 4, step, zero)


def gram_early_kernel(vi, y1, out):
    def terms(x, y):
        u = vi[x, y]
        w = y1[x, y]
        result = []
        for s in range(5):
            ws = turn_slow(w, s)
            result += [u * turn_slow(u, s), u * ws, w * ws]
        return result

    sums = diagonals(terms, 15)
    tile = jnp.zeros((8, 128), F32)
    for s in range(5):
        for m in range(3):
            tile = jnp.where(lanes() == 8 * m + s, lane_sum(sums[3 * s + m]), tile)
    out[...] = tile


def gram_late_kernel(y1, y2, early, out):
    def terms(x, y):
        u = y1[x, y]
        w = y2[x, y]
        return [u * turn_slow(w, s) for s in range(5)]

    sums = diagonals(terms, 5)
    tile = early[...]
    for s in range(5):
        tile = jnp.where(lanes() == 24 + s, lane_sum(sums[s]), tile)
    out[...] = tile


def flat_kernel(v, out):
    def turn(x, carry):
        for yb in range(4):
            out[:, x, pl.ds(8 * yb, 8), :] = jnp.swapaxes(v[x, pl.ds(8 * yb, 8)], 0, 1)
        return carry

    lax.fori_loop(0, X, turn, 0)


def column(m, j):
    return lane_sum(jnp.where(lanes() == j, m, 0.0))


def across(m, i):
    return jnp.broadcast_to(m[i : i + 1, :], (8, 128))


def times(left, right):
    total = None
    for k in range(8):
        term = column(left, k) * across(right, k)
        total = term if total is None else total + term
    return total


def flip(m):
    out = jnp.zeros((8, 128), F32)
    for k in range(8):
        out = jnp.where(lanes() == k, lane_sum(jnp.where(lanes() == rows(), across(m, k), 0.0)), out)
    return out


def solve(matrix, right):
    both = jnp.where(lanes() < 8, matrix, pltpu.roll(right, 8, axis=1))
    for k in range(8):
        col = column(both, k)
        row = across(both, k) / across(col, k)
        both = jnp.where(rows() == k, row, both - col * row)
    moved = pltpu.roll(both, 120, axis=1)
    return jnp.where(lanes() < 8, moved, 0.0)


def moments(tile, m):
    total = jnp.zeros((8, 128), F32)
    for s in range(8):
        if s <= 4:
            col = column(tile, 8 * m + s)
        else:
            col = turn_slow(column(tile, 8 * m + 8 - s), s)
        hit = (lanes() < 8) & (((rows() - lanes()) & 7) == s)
        total = jnp.where(hit, col, total)
    return total


def last_kernel(tile_ref, r0, y1, y2, sol, res, coef, sbuf, rbuf, sems):
    tile = tile_ref[...]
    m0, m1, m2, m3 = (moments(tile, m) for m in range(4))
    eye = jnp.where((lanes() == rows()) & (lanes() < 8), 1.0, 0.0)
    alpha = solve(m1, m0)
    inverse = solve(m0, eye)
    alpha_t = flip(alpha)
    m2a = times(m2, alpha)
    first = times(m1, alpha)
    rr1 = m0 - first - flip(first) + times(alpha_t, m2a)
    big = eye + times(inverse, rr1)
    big_t = flip(big)
    pq = times(big_t, times(m1, big) - m2a) + times(alpha_t, times(m3, alpha) - times(m2, big))
    alpha2 = solve(pq, rr1)
    c1 = alpha + times(big, alpha2)
    c2 = times(alpha, alpha2)
    for j in range(8):
        coef[0, j] = column(c1, j)
        coef[1, j] = column(c2, j)

    chunk = 2
    copies = []

    def tile_out(x, yb):
        at = pl.ds(8 * yb, 8)
        a = [r0[i, x, at, :] for i in range(8)]
        b = [y1[i, x, at, :] for i in range(8)]
        c = [y2[i, x, at, :] for i in range(8)]
        for j in range(8):
            s0 = s1 = t0 = t1 = None
            for i in range(8):
                p = wide(coef[0, j, pl.ds(i, 1), :])
                q = wide(coef[1, j, pl.ds(i, 1), :])
                s0 = p * a[i] if s0 is None else s0 + p * a[i]
                s1 = q * b[i] if s1 is None else s1 + q * b[i]
                t0 = p * b[i] if t0 is None else t0 + p * b[i]
                t1 = q * c[i] if t1 is None else t1 + q * c[i]
            sbuf[j, x, at, :] = s0 - s1
            rbuf[j, x, at, :] = a[j] - (t0 - t1)

    def copy(n, src, dst, which):
        part = pl.ds(n * chunk, chunk)
        return pltpu.make_async_copy(src.at[:, part], dst.at[:, part], sems.at[which, n])

    def step(n, carry):
        for xx in range(chunk):
            def inner(yb, c):
                tile_out(n * chunk + xx, yb)
                return c
            lax.fori_loop(0, 4, inner, 0)
        copy(n, sbuf, sol, 0).start()
        copy(n, rbuf, res, 1).start()
        return carry

    lax.fori_loop(0, X // chunk, step, 0)
    for n in range(X // chunk):
        copy(n, sbuf, sol, 0).wait()
        copy(n, rbuf, res, 1).wait()


def shift(x, axis, step):
    n = lax.axis_size(axis)
    return lax.ppermute(x, axis, [(i, i + step) for i in range(n) if 0 <= i + step < n])


def everywhere(x):
    for axis in ("gy", "gx", "gz"):
        bit = 1
        while bit < lax.axis_size(axis):
            n = lax.axis_size(axis)
            x = x + lax.ppermute(x, axis, [(i, i ^ bit) for i in range(n)])
            bit *= 2
    return x


def shards(rhs, stencil):
    full = (X, Y, F, Z)
    half = (HALF, Y, F, Z)
    vi, zp, zm = call(start_kernel, "k_start", [rhs, stencil], [full, (9, 8, 128), (8, 8, 128)])
    rl = shift(zp, "gz", 1)
    rr = shift(zm, "gz", -1)
    vm, vp, wz, sums, yp, ym = call(
        second_kernel, "k_second", [vi, stencil, rl, rr],
        [full, full, (9, X, Y, Z), (5, X, Y, Z), (36, 8, 128), (30, 8, 128)],
    )
    qm = shift(yp, "gy", 1)
    qp = shift(ym, "gy", -1)
    dhalf = (HALF, Y, Z)
    acc_lo, dg_lo = call(inner_kernel(0, HALF), "k_inner_lo", [vi, vm, vp, stencil, wz, sums], [half, dhalf])
    ring, xm, xp = call(
        third_kernel(True), "k_third", [vi, vm, vp, stencil, wz, rl, rr, qm, qp, sums],
        [(2, 3, X, 8, 128), (Y + 8, 8, 128), (Y + 4, 8, 128)],
    )
    tp = shift(xm, "gx", -1)
    tm = shift(xp, "gx", 1)
    acc_hi, dg_hi = call(inner_kernel(HALF, X), "k_inner_hi", [vi, vm, vp, stencil, wz, sums], [half, dhalf])
    y1, dlo, dhi, zp, zm = call(
        join_kernel(True), "k_join",
        [acc_lo, acc_hi, dg_lo, dg_hi, vi, stencil, ring, qm, qp, tp, tm],
        [full, dhalf, dhalf, (4, 8, 128), (4, 8, 128)],
    )

    rl = shift(zp, "gz", 1)
    rr = shift(zm, "gz", -1)
    (early,) = call(gram_early_kernel, "k_gram", [vi, y1], [(8, 128)])
    vm, vp, yp, ym = call(
        second_again_kernel, "k_second2", [y1, rl, rr], [full, full, (24, 8, 128), (24, 8, 128)]
    )
    qmv = shift(yp, "gy", 1)
    qpv = shift(ym, "gy", -1)
    (acc_lo,) = call(inner_again_kernel(0, HALF), "k_inner2_lo", [y1, vm, vp, stencil, wz, dlo, dhi], [half])
    ring, xm, xp = call(
        third_kernel(False), "k_third2", [y1, vm, vp, stencil, wz, rl, rr, qmv, qpv, qm, qp],
        [(2, 3, X, 8, 128), (Y + 8, 8, 128), (Y, 8, 128)],
    )
    tp = shift(xm, "gx", -1)
    tm = shift(xp, "gx", 1)
    (acc_hi,) = call(inner_again_kernel(HALF, X), "k_inner2_hi", [y1, vm, vp, stencil, wz, dlo, dhi], [half])
    (y2,) = call(
        join_kernel(False), "k_join2", [acc_lo, acc_hi, stencil, ring, qm, qp, tp, tm], [full]
    )
    (tile,) = call(gram_late_kernel, "k_gram2", [y1, y2, early], [(8, 128)])
    compact = (F, X, Y, Z)
    (y1f,) = call(flat_kernel, "k_flat1", [y1], [compact])
    (y2f,) = call(flat_kernel, "k_flat2", [y2], [compact])
    tile = everywhere(tile)
    sol, res = call(
        last_kernel, "k_last", [tile, rhs, y1f, y2f], [compact, compact],
        out_specs=[HSPEC, HSPEC],
        scratch=[
            pltpu.VMEM((2, 8, 8, 128), F32),
            pltpu.VMEM(compact, F32),
            pltpu.VMEM(compact, F32),
            pltpu.SemaphoreType.DMA((2, X // 2)),
        ],
        limit=14,
    )
    return sol, res


def solution(mesh):
    placed = P(None, "gx", "gy", "gz")
    return jax.shard_map(
        shards, mesh=mesh, in_specs=(placed, placed), out_specs=(placed, placed), check_vma=False
    )
```

```python
import jax
import jax.numpy as jnp
from jax import lax
from jax.experimental import pallas as pl
from jax.experimental.pallas import tpu as pltpu
from jax.sharding import PartitionSpec as P

F32 = jnp.float32
X, Y, Z, F = 16, 32, 128, 8
FORWARD = [
    (a, b, c) for a in (-1, 0, 1) for b in (-1, 0, 1) for c in (-1, 0, 1) if (a, b, c) > (0, 0, 0)
]
OFF = {k + 1: o for k, o in enumerate(FORWARD)}
ZPLUS = [k for k in OFF if OFF[k][2] == 1]
ZMINUS = [k for k in OFF if OFF[k][2] == -1]
YPLUS = [k for k in OFF if OFF[k][1] == 1]
YMINUS = [k for k in OFF if OFF[k][1] == -1]
XPLUS = [k for k in OFF if OFF[k][0] == 1]
ZSHIFTED = ZPLUS + ZMINUS
WZ_AT = {k: i for i, k in enumerate(ZSHIFTED)}
PAIRS = tuple(zip(ZPLUS, ZMINUS + [None]))
GROUPS = ((0, 1), (1, -1), (1, 0), (1, 1))
SHIFT_AT = {0: 0, -1: 1, 1: 2}

VSPEC = pl.BlockSpec(memory_space=pltpu.VMEM)
HSPEC = pl.BlockSpec(memory_space=pl.ANY)
MIB = 1024 * 1024


def call(body, name, ins, outs, after=(), aliases=None, scratch=(), in_specs=None, out_specs=None, limit=8):
    count = len(ins)

    def run(*refs):
        body(*refs[:count], *refs[count + len(after):])

    return pl.pallas_call(
        run,
        name=name,
        out_shape=[jax.ShapeDtypeStruct(s, F32) for s in outs],
        in_specs=(in_specs or [VSPEC] * count) + [HSPEC] * len(after),
        out_specs=out_specs or [VSPEC] * len(outs),
        input_output_aliases=aliases or {},
        scratch_shapes=list(scratch),
        compiler_params=pltpu.CompilerParams(vmem_limit_bytes=limit * MIB),
    )(*ins, *after)


def lanes():
    return lax.broadcasted_iota(jnp.int32, (8, 128), 1)


def rows():
    return lax.broadcasted_iota(jnp.int32, (8, 128), 0)


def roll(v, shift):
    shift %= 128
    return pltpu.roll(v, shift, axis=1) if shift else v


def spot(x, y):
    return (x % 4) * 32 + y


def with_ends(value, ends):
    before = roll(jnp.where(lanes() == 127, ends, value), 1)
    after = roll(jnp.where(lanes() == 0, ends, value), -1)
    return before, after


def clear_if(condition, *outs):
    @pl.when(condition)
    def _():
        for ref in outs:
            ref[...] = jnp.zeros(ref.shape, F32)


def at_first(axis):
    return lax.axis_index(axis) == 0


def at_last(axis):
    return lax.axis_index(axis) == lax.axis_size(axis) - 1


def pack_group(field, g, zp, zm):
    high = jnp.zeros((8, 128), F32)
    low = jnp.zeros((8, 128), F32)
    for xx in range(4):
        for y in range(Y):
            at = spot(xx, y)
            v = roll(field[4 * g + xx, y], at + 1)
            high = jnp.where(lanes() == at, v, high)
            low = jnp.where(lanes() == (at + 1) % 128, v, low)
    zp[g] = high
    zm[g] = low


def pack_columns(field, zp, zm):
    def group(g, carry):
        pack_group(field, g, zp, zm)
        return carry

    lax.fori_loop(0, 4, group, 0)


def start_kernel(rhs, stencil, rc, st, vi, zp, zm, sem_r, sem_s):
    def part(g):
        at = pl.ds(4 * g, 4)
        return pltpu.make_async_copy(rhs.at[:, at], rc.at[:, at], sem_r.at[g])

    def field(k):
        return pltpu.make_async_copy(stencil.at[k], st.at[k], sem_s.at[k])

    order = [k for pair in PAIRS for k in pair if k is not None]
    order += [k for k in range(14) if k not in order]
    for g in range(4):
        part(g).start()
    for k in order:
        field(k).start()

    def group(g, carry):
        part(g).wait()
        for xx in range(4):
            x = 4 * g + xx
            for yb in range(4):
                vi[x, pl.ds(8 * yb, 8)] = jnp.swapaxes(rc[:, x, pl.ds(8 * yb, 8), :], 0, 1)
        pack_group(vi, g, zp, zm)
        return carry

    lax.fori_loop(0, 4, group, 0)
    for k in order:
        field(k).wait()
    for j, (up, down) in enumerate(PAIRS):
        out = jnp.zeros((8, 128), F32)
        for x in range(X):
            for yb in range(4):
                at = 8 * x + 2 * yb
                w = st[up, x, pl.ds(8 * yb, 8), :]
                if down is not None:
                    w = jnp.where(lanes() == 0, st[down, x, pl.ds(8 * yb, 8), :], w)
                out = jnp.where((lanes() == at) | (lanes() == at + 1), roll(w, at + 1), out)
        zp[4 + j] = out
        zm[4 + j] = out
    clear_if(at_last("gz"), zp)
    clear_if(at_first("gz"), zm)


def even():
    return (lanes() & 1) == 0


def merged(rl, rr, g):
    left, right = rl[g], rr[g]
    return jnp.where(even(), left, right), jnp.where(even(), right, left)


def ends_of(pair, at):
    return roll(pair[at % 2], -(at + 1))


def shift_fields(vi, rl, rr, vm, vp):
    def group(g, carry):
        pair = merged(rl, rr, g)
        for xx in range(4):
            for part in range(0, Y, 16):
                ys = range(part, part + 16)
                ends = [ends_of(pair, spot(xx, y)) for y in ys]
                for y, end in zip(ys, ends):
                    before, after = with_ends(vi[4 * g + xx, y], end)
                    vm[4 * g + xx, y] = before
                    vp[4 * g + xx, y] = after
        return carry

    lax.fori_loop(0, 4, group, 0)


def shifted_couplings(st, ends, j, spots):
    up, down = PAIRS[j]
    tiles = [roll(ends[j], -(8 * x + 2 * yb + 1)) for x, yb in spots]
    result = []
    for tile, (x, yb) in zip(tiles, spots):
        w = st[up, x, pl.ds(8 * yb, 8), :]
        moved = {up: roll(jnp.where(lanes() == 127, tile, w), 1)}
        if down is not None:
            w = st[down, x, pl.ds(8 * yb, 8), :]
            moved[down] = roll(jnp.where(lanes() == 0, tile, w), -1)
        result.append(moved)
    return result


def edge_rows(vi, rl, rr, yp, ym):
    for x in range(X):
        yp[x] = vi[x, Y - 1]
        ym[x] = vi[x, 0]
    for g in range(4):
        for i, tile in enumerate(merged(rl, rr, g)):
            yp[16 + 2 * g + i] = tile
            ym[16 + 2 * g + i] = tile


def coupling_ends(rl, rr):
    return [jnp.where(even(), rl[4 + j], rr[4 + j]) for j in range(5)]


def edge_kernel(vi, st, rl, rr, yp, ym):
    edge_rows(vi, rl, rr, yp, ym)
    ends = coupling_ends(rl, rr)
    for ref, keys, y in ((yp, YPLUS, Y - 1), (ym, YMINUS, 0)):
        rows_of = {}
        for j, pair in enumerate(PAIRS):
            if pair[0] in keys or pair[1] in keys:
                moved = shifted_couplings(st, ends, j, [(x, y // 8) for x in range(X)])
                for x in range(X):
                    rows_of.update({(k, x): tile for k, tile in moved[x].items()})
        for i, k in enumerate(keys):
            for x in range(X):
                r = 16 * i + x
                if k in WZ_AT:
                    row = rows_of[k, x][y % 8 : y % 8 + 1, :]
                else:
                    row = st[k, x, pl.ds(y, 1), :]
                ref[24 + r // 8, pl.ds(r % 8, 1), :] = row
    clear_if(at_last("gy"), yp)
    clear_if(at_first("gy"), ym)


def edge_again_kernel(vi, rl, rr, yp, ym):
    edge_rows(vi, rl, rr, yp, ym)
    clear_if(at_last("gy"), yp)
    clear_if(at_first("gy"), ym)


def shift_kernel(vi, st, rl, rr, vm, vp, wz, sums):
    shift_fields(vi, rl, rr, vm, vp)
    ends = coupling_ends(rl, rr)
    for j in range(5):
        for x in range(0, X, 4):
            spots = [(x + i, yb) for i in range(4) for yb in range(4)]
            for (xx, yb), moved in zip(spots, shifted_couplings(st, ends, j, spots)):
                for k, tile in moved.items():
                    wz[WZ_AT[k], xx, pl.ds(8 * yb, 8), :] = tile

    def behind(k, x, yb):
        if k in WZ_AT:
            return wz[WZ_AT[k], x, pl.ds(8 * yb, 8), :]
        return st[k, x, pl.ds(8 * yb, 8), :]

    def add_up(x, carry):
        for yb in range(4):
            total = st[0, x, pl.ds(8 * yb, 8), :]
            for k in OFF:
                total = total + st[k, x, pl.ds(8 * yb, 8), :]
            sums[4, x, pl.ds(8 * yb, 8), :] = total + behind(1, x, yb)
            for i, (a, b) in enumerate(GROUPS):
                keys = [k for k in OFF if OFF[k][:2] == (a, b)]
                sums[i, x, pl.ds(8 * yb, 8), :] = (
                    behind(keys[0], x, yb) + behind(keys[1], x, yb) + behind(keys[2], x, yb)
                )
        return carry

    lax.fori_loop(0, X, add_up, 0)


def behind_row(st, wz, k, x, y):
    if k in WZ_AT:
        return wz[WZ_AT[k], x, pl.ds(y, 1), :]
    return st[k, x, pl.ds(y, 1), :]


def wide(row):
    return jnp.broadcast_to(row, (8, 128))


def plane(x, first, last, fields, st, wz, acc_ref, at, diag_of):
    cache = {}

    def v(s, dx, y):
        key = (s, dx, y)
        if key not in cache:
            cache[key] = fields[SHIFT_AT[s]][x + dx, y]
        return cache[key]

    coef = {}

    def ahead(k, y):
        if OFF[k][2] == 0:
            if (k, 0, y) not in coef:
                coef[k, 0, y] = wide(st[k, x, pl.ds(y, 1), :])
            return coef[k, 0, y]
        return wide(st[k, x, pl.ds(y, 1), :])

    def behind(k, a, y):
        if k not in WZ_AT:
            if (k, a, y) not in coef:
                coef[k, a, y] = wide(st[k, x - a, pl.ds(y, 1), :])
            return coef[k, a, y]
        return wide(wz[WZ_AT[k], x - a, pl.ds(y, 1), :])

    for y in range(Y):
        parts = [None, None]
        n = 0
        for k, (a, b, c) in OFF.items():
            if 0 <= y + b < Y and not (a == 1 and last):
                term = ahead(k, y) * v(c, a, y + b)
                parts[n % 2] = term if parts[n % 2] is None else parts[n % 2] + term
                n += 1
            if 0 <= y - b < Y and not (a == 1 and first):
                term = behind(k, a, y - b) * v(-c, -a, y - b)
                parts[n % 2] = term if parts[n % 2] is None else parts[n % 2] + term
                n += 1
        acc_ref[at, y] = wide(diag_of(x, y, first)) * v(0, 0, y) - (parts[0] + parts[1])


def interior(fields, st, wz, acc_ref, diag_of):
    plane(0, True, False, fields, st, wz, acc_ref, 0, diag_of)

    def step(x, carry):
        plane(x, False, False, fields, st, wz, acc_ref, x, diag_of)
        return carry

    lax.fori_loop(1, X - 1, step, 0)
    plane(X - 1, False, True, fields, st, wz, acc_ref, X - 1, diag_of)


def inner_kernel(vi, vm, vp, st, wz, sums, acc, diag):
    def diag_of(x, y, first):
        total = sums[4, x, pl.ds(y, 1), :]
        if y > 0:
            total = total + sums[0, x, pl.ds(y - 1, 1), :]
        if not first:
            total = total + sums[2, x - 1, pl.ds(y, 1), :]
            if y > 0:
                total = total + sums[3, x - 1, pl.ds(y - 1, 1), :]
            if y < Y - 1:
                total = total + sums[1, x - 1, pl.ds(y + 1, 1), :]
        diag[x, pl.ds(y, 1), :] = total
        return total

    interior((vi, vm, vp), st, wz, acc, diag_of)


def inner_again_kernel(vi, vm, vp, st, wz, diag, acc):
    interior((vi, vm, vp), st, wz, acc, lambda x, y, first: diag[x, pl.ds(y, 1), :])


def ring_row(ref, keys, k, x):
    r = 16 * keys.index(k) + x
    return ref[24 + r // 8, pl.ds(r % 8, 1), :]


def third_kernel(with_diag):
    def body(*refs):
        if with_diag:
            vi, vm, vp, st, wz, rl, rr, qm, qp, sums, ring, xm, xp = refs
            qmw, qpw = qm, qp
        else:
            vi, vm, vp, st, wz, rl, rr, qm, qp, qmw, qpw, ring, xm, xp = refs
        for side, q, y in ((0, qm, Y - 1), (1, qp, 0)):
            for x in range(X):
                g = 16 + 2 * (x // 4)
                before, after = with_ends(q[x], ends_of((q[g], q[g + 1]), spot(x, y)))
                ring[side, 0, x] = q[x]
                ring[side, 1, x] = before
                ring[side, 2, x] = after
        xm[0] = qm[0]
        for y in range(Y):
            xm[1 + y] = vi[0, y]
        xm[Y + 1] = qp[0]
        for i, tile in enumerate((*merged(rl, rr, 0), qm[16], qm[17], qp[16], qp[17])):
            xm[Y + 2 + i] = tile
        last = X - 1
        for y in range(Y):
            total = None
            for k in XPLUS:
                _, b, c = OFF[k]
                s = SHIFT_AT[-c]
                if y - b < 0:
                    term = wide(ring_row(qmw, YPLUS, k, last)) * ring[0, s, last]
                elif y - b >= Y:
                    term = wide(ring_row(qpw, YMINUS, k, last)) * ring[1, s, last]
                else:
                    term = wide(behind_row(st, wz, k, last, y - b)) * (vi, vm, vp)[s][last, y - b]
                total = term if total is None else total + term
            xp[y] = total
            if with_diag:
                row = sums[2, last, pl.ds(y, 1), :]
                if y > 0:
                    row = row + sums[3, last, pl.ds(y - 1, 1), :]
                else:
                    for k in (11, 12, 13):
                        row = row + ring_row(qmw, YPLUS, k, last)
                if y < Y - 1:
                    row = row + sums[1, last, pl.ds(y + 1, 1), :]
                else:
                    for k in (5, 6, 7):
                        row = row + ring_row(qpw, YMINUS, k, last)
                xp[Y + y // 8, pl.ds(y % 8, 1), :] = row
        clear_if(at_first("gx"), xm)
        clear_if(at_last("gx"), xp)

    return body


def finish_edges(acc, st, ring, qmw, qpw, tp, tm, extra):
    last = X - 1
    far = {}

    def far_at(s, y):
        if (0, y) not in far:
            base, at = (Y + 2, y) if 0 <= y < Y else ((Y + 4, Y - 1) if y < 0 else (Y + 6, 0))
            far[0, y] = tp[y + 1]
            far[-1, y], far[1, y] = with_ends(tp[y + 1], ends_of((tp[base], tp[base + 1]), at))
        return far[s, y]

    for x in range(X):
        for y in range(Y) if x in (0, last) else (0, Y - 1):
            total = None
            for k, (a, b, c) in OFF.items():
                terms = []
                if x + a == X:
                    terms.append(wide(st[k, x, pl.ds(y, 1), :]) * far_at(c, y + b))
                elif y + b < 0:
                    terms.append(wide(st[k, x, pl.ds(y, 1), :]) * ring[0, SHIFT_AT[c], x + a])
                elif y + b >= Y:
                    terms.append(wide(st[k, x, pl.ds(y, 1), :]) * ring[1, SHIFT_AT[c], x + a])
                if x - a >= 0:
                    if y - b < 0:
                        terms.append(
                            wide(ring_row(qmw, YPLUS, k, x - a)) * ring[0, SHIFT_AT[-c], x - a]
                        )
                    elif y - b >= Y:
                        terms.append(
                            wide(ring_row(qpw, YMINUS, k, x - a)) * ring[1, SHIFT_AT[-c], x - a]
                        )
                for term in terms:
                    total = term if total is None else total + term
            if x == 0:
                total = tm[y] if total is None else total + tm[y]
            value = acc[x, y] - total
            fix = extra(x, y) if extra is not None else None
            acc[x, y] = value if fix is None else value + fix


def join_kernel(acc_in, diag_in, vi, st, ring, qm, qp, tp, tm, acc, diag, zp, zm):
    def fix(x, y):
        row = None
        if y == 0:
            for k in (2, 3, 4):
                r = ring_row(qm, YPLUS, k, x)
                row = r if row is None else row + r
            if x > 0:
                for k in (11, 12, 13):
                    row = row + ring_row(qm, YPLUS, k, x - 1)
        if y == Y - 1 and x > 0:
            for k in (5, 6, 7):
                r = ring_row(qp, YMINUS, k, x - 1)
                row = r if row is None else row + r
        if x == 0:
            r = tm[Y + y // 8, pl.ds(y % 8, 1), :]
            row = r if row is None else row + r
        if row is None:
            return None
        diag[x, pl.ds(y, 1), :] = diag[x, pl.ds(y, 1), :] + row
        return wide(row) * vi[x, y]

    finish_edges(acc, st, ring, qm, qp, tp, tm, fix)
    pack_columns(acc, zp, zm)
    clear_if(at_last("gz"), zp)
    clear_if(at_first("gz"), zm)


def turn_flat(v, out, x):
    for yb in range(4):
        out[:, x, pl.ds(8 * yb, 8), :] = jnp.swapaxes(v[x, pl.ds(8 * yb, 8)], 0, 1)


def flat_kernel(v, out):
    def turn(x, carry):
        turn_flat(v, out, x)
        return carry

    lax.fori_loop(0, X, turn, 0)


PRODUCTS = [(i, j) for i in range(8) for j in range(i, 8)]


def gram(u, v):
    def step(n, carry):
        x, at = n // 4, pl.ds((n % 4) * 8, 8)
        a = [u[i, x, at, :] for i in range(8)]
        b = a if v is u else [v[i, x, at, :] for i in range(8)]
        return tuple(c + a[i] * b[j] for c, (i, j) in zip(carry, PRODUCTS))

    return lax.fori_loop(0, 4 * X, step, tuple(jnp.zeros((8, 128), F32) for _ in PRODUCTS))


def place(tile, sums, m):
    held = dict(zip(PRODUCTS, sums))
    held = {p: jnp.sum(s, axis=1, keepdims=True) for p, s in held.items()}
    for i in range(8):
        row = jnp.zeros((8, 128), F32)
        for j in range(8):
            row = jnp.where(lanes() == 8 * m + j, held[min(i, j), max(i, j)], row)
        row = jnp.broadcast_to(jnp.sum(row, axis=0, keepdims=True), (8, 128))
        mine = (rows() == i) & (lanes() >= 8 * m) & (lanes() < 8 * m + 8)
        tile = jnp.where(mine, row, tile)
    return tile


def gram_first_kernel(r0, out):
    out[...] = place(jnp.zeros((8, 128), F32), gram(r0, r0), 0)


def gram_second_kernel(r0, y1, early, flat, out):
    flat_kernel(y1, flat)
    tile = place(early[...], gram(r0, flat), 1)
    out[...] = place(tile, gram(flat, flat), 2)


def late_kernel(acc_in, st, ring, qm, qp, tp, tm, y1, early, acc, flat, out):
    finish_edges(acc, st, ring, qm, qp, tp, tm, None)
    flat_kernel(acc, flat)
    out[...] = place(early[...], gram(y1, flat), 3)


def differences_kernel(r0, y1, y2, d0, d1):
    def step(x, carry):
        for i in range(8):
            d0[i, x] = r0[i, x] - y1[i, x]
            d1[i, x] = y1[i, x] - y2[i, x]
        return carry

    lax.fori_loop(0, X, step, 0)


def entry(col, i):
    return jnp.broadcast_to(col[i : i + 1, :], (8, 128))


def times(left, right):
    result = []
    for j in range(8):
        total = None
        for k in range(8):
            term = left[k] * entry(right[j], k)
            total = term if total is None else total + term
        result.append(total)
    return result


def flip(m):
    result = []
    for j in range(8):
        out = entry(m[0], j)
        for i in range(1, 8):
            out = jnp.where(rows() == i, entry(m[i], j), out)
        result.append(out)
    return result


def plus(left, right):
    return [a + b for a, b in zip(left, right)]


def minus(left, right):
    return [a - b for a, b in zip(left, right)]


def solve(matrix, right):
    a = list(matrix)
    r = list(right)
    for k in range(8):
        inverse = 1.0 / entry(a[k], k)
        here = rows() == k
        for cols, js in ((a, range(k + 1, 8)), (r, range(8))):
            for j in js:
                f = entry(cols[j], k) * inverse
                cols[j] = jnp.where(here, f, cols[j] - a[k] * f)
    return r


def moments(tile, m):
    return [jnp.broadcast_to(tile[:, 8 * m + j : 8 * m + j + 1], (8, 128)) for j in range(8)]


def coefficients(tile):
    m0, m1, m2, m3 = (moments(tile, m) for m in range(4))
    eye = [jnp.where(rows() == j, 1.0, 0.0) for j in range(8)]
    alpha = solve(m1, m0)
    inverse = solve(m0, eye)
    alpha_t = flip(alpha)
    m2a = times(m2, alpha)
    first = times(m1, alpha)
    rr1 = plus(minus(minus(m0, first), flip(first)), times(alpha_t, m2a))
    big = plus(eye, times(inverse, rr1))
    pq = plus(
        times(flip(big), minus(times(m1, big), m2a)),
        times(alpha_t, minus(times(m3, alpha), times(m2, big))),
    )
    alpha2 = solve(pq, rr1)
    return plus(alpha, times(big, alpha2)), times(alpha, alpha2)


def last_kernel(tile_ref, r0, y1, d0, d1, sol, res, coef, sbuf, rbuf, sems):
    c1, c2 = coefficients(tile_ref[...])
    for j in range(8):
        coef[0, j] = c1[j]
        coef[1, j] = c1[j] - c2[j]
        coef[2, j] = c2[j]

    def tile_out(x, yb):
        at = pl.ds(8 * yb, 8)
        a = [d0[i, x, at, :] for i in range(8)]
        b = [y1[i, x, at, :] for i in range(8)]
        c = [d1[i, x, at, :] for i in range(8)]
        for j in range(8):
            sums = []
            for m, field in enumerate((a, b, c)):
                total = None
                for i in range(8):
                    term = wide(coef[m, j, pl.ds(i, 1), :]) * field[i]
                    total = term if total is None else total + term
                sums.append(total)
            sbuf[j, x, at, :] = sums[0] + sums[1]
            rbuf[j, x, at, :] = r0[j, x, at, :] - (sums[1] + sums[2])

    def copy(n, src, dst, which):
        part = pl.ds(n * 2, 2)
        return pltpu.make_async_copy(src.at[:, part], dst.at[:, part], sems.at[which, n])

    def step(n, carry):
        def inner(t, c):
            tile_out(n * 2 + t // 4, t % 4)
            return c

        lax.fori_loop(0, 8, inner, 0)
        copy(n, sbuf, sol, 0).start()
        copy(n, rbuf, res, 1).start()
        return carry

    lax.fori_loop(0, X // 2, step, 0)
    for n in range(X // 2):
        copy(n, sbuf, sol, 0).wait()
        copy(n, rbuf, res, 1).wait()


def shift(x, axis, step):
    n = lax.axis_size(axis)
    return lax.ppermute(x, axis, [(i, (i + step) % n) for i in range(n)])


def everywhere(x):
    for axis, bits in (("gy", (1, 2, 6)), ("gx", (1, 3)), ("gz", (1, 3))):
        n = lax.axis_size(axis)
        for bit in bits:
            x = x + lax.ppermute(x, axis, [(i, i ^ bit) for i in range(n)])
    return x


def shards(rhs, stencil):
    full = (X, Y, F, Z)
    compact = (F, X, Y, Z)
    tile = (8, 128)
    dma = pltpu.SemaphoreType.DMA
    rc, st, vi, zp, zm = call(
        start_kernel, "k_start", [rhs, stencil],
        [compact, (14, X, Y, Z), full, (9, *tile), (9, *tile)],
        in_specs=[HSPEC] * 2, scratch=[dma((4,)), dma((14,))],
    )
    rl = shift(zp, "gz", 1)
    rr = shift(zm, "gz", -1)
    (g0,) = call(gram_first_kernel, "k_gram0", [rc], [tile])
    yp, ym = call(edge_kernel, "k_edge", [vi, st, rl, rr], [(36, *tile), (30, *tile)], after=[g0])
    qm = shift(yp, "gy", 1)
    qp = shift(ym, "gy", -1)
    vm, vp, wz, sums = call(
        shift_kernel, "k_shift", [vi, st, rl, rr], [full, full, (9, X, Y, Z), (5, X, Y, Z)]
    )
    ring, xm, xp = call(
        third_kernel(True), "k_third", [vi, vm, vp, st, wz, rl, rr, qm, qp, sums],
        [(2, 3, X, *tile), (Y + 8, *tile), (Y + 4, *tile)],
    )
    tp = shift(xm, "gx", -1)
    tm = shift(xp, "gx", 1)
    acc, diag = call(inner_kernel, "k_inner", [vi, vm, vp, st, wz, sums], [full, (X, Y, Z)])
    y1, diag, zp, zm = call(
        join_kernel, "k_join", [acc, diag, vi, st, ring, qm, qp, tp, tm],
        [full, (X, Y, Z), (4, *tile), (4, *tile)], aliases={0: 0, 1: 1},
    )

    rl = shift(zp, "gz", 1)
    rr = shift(zm, "gz", -1)
    y1f, g2 = call(gram_second_kernel, "k_gram12", [rc, y1, g0], [compact, tile])
    yp, ym = call(
        edge_again_kernel, "k_edge2", [y1, rl, rr], [(24, *tile), (24, *tile)], after=[g2]
    )
    qmv = shift(yp, "gy", 1)
    qpv = shift(ym, "gy", -1)
    vm, vp = call(shift_fields, "k_shift2", [y1, rl, rr], [full, full])
    ring, xm, xp = call(
        third_kernel(False), "k_third2", [y1, vm, vp, st, wz, rl, rr, qmv, qpv, qm, qp],
        [(2, 3, X, *tile), (Y + 8, *tile), (Y, *tile)],
    )
    tp = shift(xm, "gx", -1)
    tm = shift(xp, "gx", 1)
    (acc,) = call(inner_again_kernel, "k_inner2", [y1, vm, vp, st, wz, diag], [full])
    _, y2f, moment = call(
        late_kernel, "k_late", [acc, st, ring, qm, qp, tp, tm, y1f, g2],
        [full, compact, tile], aliases={0: 0},
    )
    d0, d1 = call(differences_kernel, "k_diff", [rc, y1f, y2f], [compact, compact])
    moment = everywhere(moment)
    sol, res = call(
        last_kernel, "k_last", [moment, rc, y1f, d0, d1], [compact, compact],
        out_specs=[HSPEC, HSPEC],
        scratch=[
            pltpu.VMEM((3, 8, *tile), F32),
            pltpu.VMEM(compact, F32),
            pltpu.VMEM(compact, F32),
            dma((2, X // 2)),
        ],
        limit=14,
    )
    return sol, res


def solution(mesh):
    placed = P(None, "gx", "gy", "gz")
    return jax.shard_map(
        shards, mesh=mesh, in_specs=(placed, placed), out_specs=(placed, placed), check_vma=False
    )
```

```python
import jax
import jax.numpy as jnp
from jax import lax
from jax.experimental import pallas as pl
from jax.experimental.pallas import tpu as pltpu
from jax.sharding import PartitionSpec as P

F32 = jnp.float32
X, Y, Z, F = 16, 32, 128, 8
FORWARD = [
    (a, b, c) for a in (-1, 0, 1) for b in (-1, 0, 1) for c in (-1, 0, 1) if (a, b, c) > (0, 0, 0)
]
OFF = {k + 1: o for k, o in enumerate(FORWARD)}
ZPLUS = [k for k in OFF if OFF[k][2] == 1]
ZMINUS = [k for k in OFF if OFF[k][2] == -1]
YPLUS = [k for k in OFF if OFF[k][1] == 1]
YMINUS = [k for k in OFF if OFF[k][1] == -1]
XPLUS = [k for k in OFF if OFF[k][0] == 1]
ZSHIFTED = ZPLUS + ZMINUS
WZ_AT = {k: i for i, k in enumerate(ZSHIFTED)}
PAIRS = tuple(zip(ZPLUS, ZMINUS + [None]))
GROUPS = ((0, 1), (1, -1), (1, 0), (1, 1))
SHIFT_AT = {0: 0, -1: 1, 1: 2}

VSPEC = pl.BlockSpec(memory_space=pltpu.VMEM)
HSPEC = pl.BlockSpec(memory_space=pl.ANY)
FAR = pl.BlockSpec(memory_space=pltpu.HBM)
MIB = 1024 * 1024
START_LIMIT = 48


def call(body, name, ins, outs, after=(), aliases=None, scratch=(), in_specs=None, out_specs=None, limit=8):
    count = len(ins)

    def run(*refs):
        body(*refs[:count], *refs[count + len(after):])

    return pl.pallas_call(
        run,
        name=name,
        out_shape=[jax.ShapeDtypeStruct(s, F32) for s in outs],
        in_specs=(in_specs or [VSPEC] * count) + [HSPEC] * len(after),
        out_specs=out_specs or [VSPEC] * len(outs),
        input_output_aliases=aliases or {},
        scratch_shapes=list(scratch),
        compiler_params=pltpu.CompilerParams(vmem_limit_bytes=limit * MIB),
    )(*ins, *after)


def lanes():
    return lax.broadcasted_iota(jnp.int32, (8, 128), 1)


def rows():
    return lax.broadcasted_iota(jnp.int32, (8, 128), 0)


def roll(v, shift):
    shift %= 128
    return pltpu.roll(v, shift, axis=1) if shift else v


def spot(x, y):
    return (x % 4) * 32 + y


def with_ends(value, ends):
    before = jnp.where(lanes() == 0, ends, roll(value, 1))
    after = jnp.where(lanes() == 127, ends, roll(value, -1))
    return before, after


def clear_if(condition, *outs):
    @pl.when(condition)
    def _():
        for ref in outs:
            ref[...] = jnp.zeros(ref.shape, F32)


def at_first(axis):
    return lax.axis_index(axis) == 0


def at_last(axis):
    return lax.axis_index(axis) == lax.axis_size(axis) - 1


def pack_group(field, g, zp, zm):
    high = jnp.zeros((8, 128), F32)
    low = jnp.zeros((8, 128), F32)
    for xx in range(4):
        for y in range(Y):
            at = spot(xx, y)
            v = roll(field[4 * g + xx, y], at + 1)
            high = jnp.where(lanes() == at, v, high)
            low = jnp.where(lanes() == (at + 1) % 128, v, low)
    zp[g] = high
    zm[g] = low


def pack_columns(field, zp, zm):
    def group(g, carry):
        pack_group(field, g, zp, zm)
        return carry

    lax.fori_loop(0, 4, group, 0)


def start_kernel(rhs, stencil, rc, vi, zp, zm, st, sem_r, sem_s):
    def part(g):
        at = pl.ds(4 * g, 4)
        return pltpu.make_async_copy(rhs.at[:, at], rc.at[:, at], sem_r.at[g])

    def field(k):
        at = WZ_AT[k]
        return pltpu.make_async_copy(stencil.at[k], st.at[at], sem_s.at[at])

    order = [k for pair in PAIRS for k in pair if k is not None]
    for g in range(4):
        part(g).start()
    for k in order:
        field(k).start()

    def group(g, carry):
        part(g).wait()
        for xx in range(4):
            x = 4 * g + xx
            for yb in range(4):
                vi[x, pl.ds(8 * yb, 8)] = jnp.swapaxes(rc[:, x, pl.ds(8 * yb, 8), :], 0, 1)
        pack_group(vi, g, zp, zm)
        return carry

    lax.fori_loop(0, 4, group, 0)
    for k in order:
        field(k).wait()
    for j, (up, down) in enumerate(PAIRS):
        out = jnp.zeros((8, 128), F32)
        for x in range(X):
            for yb in range(4):
                at = 8 * x + 2 * yb
                w = st[WZ_AT[up], x, pl.ds(8 * yb, 8), :]
                if down is not None:
                    w = jnp.where(lanes() == 0, st[WZ_AT[down], x, pl.ds(8 * yb, 8), :], w)
                out = jnp.where((lanes() == at) | (lanes() == at + 1), roll(w, at + 1), out)
        zp[4 + j] = out
        zm[4 + j] = out
    clear_if(at_last("gz"), zp)
    clear_if(at_first("gz"), zm)


def even():
    return (lanes() & 1) == 0


def merged(rl, rr, g):
    left, right = roll(rl[g], 2), rr[g]
    return jnp.where(even(), left, right), jnp.where(even(), right, left)


def ends_of(pair, at):
    return roll(pair[at % 2], -(at + 2))


def coupling_ends(rl, rr):
    return [jnp.where(even(), roll(rl[4 + j], 2), rr[4 + j]) for j in range(5)]


def coupling_end(ends, j, x, yb):
    return roll(ends[j], -(8 * x + 2 * yb + 2))


def roll_rows(vi, vm, vp, x):
    for y in range(Y):
        v = vi[x, y]
        vm[x, y] = roll(v, 1)
        vp[x, y] = roll(v, -1)


def roll_fields(vi, vm, vp):
    def step(n, carry):
        for i in range(4):
            roll_rows(vi, vm, vp, 4 * n + i)
        return carry

    lax.fori_loop(0, X // 4, step, 0)


def roll_kernel(vi, st, vm, vp, wz):
    def step(n, carry):
        for i in range(4):
            x = 4 * n + i
            roll_rows(vi, vm, vp, x)
            for k in ZSHIFTED:
                for yb in range(4):
                    at = pl.ds(8 * yb, 8)
                    wz[WZ_AT[k], x, at, :] = roll(st[k, x, at, :], OFF[k][2])
        return carry

    lax.fori_loop(0, X // 4, step, 0)


def put_ends(rl, rr, vm, vp):
    first, last = lanes() == 0, lanes() == 127

    def group(g, carry):
        pair = merged(rl, rr, g)
        for xx in range(4):
            for y in range(Y):
                end = ends_of(pair, spot(xx, y))
                pltpu.store(vm.at[4 * g + xx, y], end, mask=first)
                pltpu.store(vp.at[4 * g + xx, y], end, mask=last)
        return carry

    lax.fori_loop(0, 4, group, 0)


def ends_kernel(vm_in, vp_in, wz_in, st, rl, rr, vm, vp, wz, sums):
    put_ends(rl, rr, vm, vp)
    ends = coupling_ends(rl, rr)
    first, last = lanes() == 0, lanes() == 127
    for j, pair in enumerate(PAIRS):
        for x in range(X):
            for yb in range(4):
                end = coupling_end(ends, j, x, yb)
                for k, mask in zip(pair, (first, last)):
                    if k is not None:
                        pltpu.store(wz.at[WZ_AT[k], x, pl.ds(8 * yb, 8), :], end, mask=mask)

    def behind(k, x, yb):
        if k in WZ_AT:
            return wz[WZ_AT[k], x, pl.ds(8 * yb, 8), :]
        return st[k, x, pl.ds(8 * yb, 8), :]

    def add_up(x, carry):
        for yb in range(4):
            total = st[0, x, pl.ds(8 * yb, 8), :]
            for k in OFF:
                total = total + st[k, x, pl.ds(8 * yb, 8), :]
            sums[4, x, pl.ds(8 * yb, 8), :] = total + behind(1, x, yb)
            for i, (a, b) in enumerate(GROUPS):
                keys = [k for k in OFF if OFF[k][:2] == (a, b)]
                sums[i, x, pl.ds(8 * yb, 8), :] = (
                    behind(keys[0], x, yb) + behind(keys[1], x, yb) + behind(keys[2], x, yb)
                )
        return carry

    lax.fori_loop(0, X, add_up, 0)


def ends_again_kernel(vm_in, vp_in, rl, rr, vm, vp):
    put_ends(rl, rr, vm, vp)


def edge_rows(vi, rl, rr, yp, ym):
    for x in range(X):
        yp[x] = vi[x, Y - 1]
        ym[x] = vi[x, 0]
    for g in range(4):
        for i, tile in enumerate(merged(rl, rr, g)):
            yp[16 + 2 * g + i] = tile
            ym[16 + 2 * g + i] = tile


def edge_kernel(vi, st, wz, rl, rr, yp, ym):
    edge_rows(vi, rl, rr, yp, ym)
    ends = coupling_ends(rl, rr)
    for ref, keys, y in ((yp, YPLUS, Y - 1), (ym, YMINUS, 0)):
        rows_of = {}
        for j, pair in enumerate(PAIRS):
            for x in range(X):
                for k, edge in zip(pair, (0, 127)):
                    if k in keys:
                        end = coupling_end(ends, j, x, y // 8)
                        w = wz[WZ_AT[k], x, pl.ds(8 * (y // 8), 8), :]
                        rows_of[k, x] = jnp.where(lanes() == edge, end, w)
        for i, k in enumerate(keys):
            for x in range(X):
                r = 16 * i + x
                if k in WZ_AT:
                    row = rows_of[k, x][y % 8 : y % 8 + 1, :]
                else:
                    row = st[k, x, pl.ds(y, 1), :]
                ref[24 + r // 8, pl.ds(r % 8, 1), :] = row
    clear_if(at_last("gy"), yp)
    clear_if(at_first("gy"), ym)


def edge_again_kernel(vi, rl, rr, yp, ym):
    edge_rows(vi, rl, rr, yp, ym)
    clear_if(at_last("gy"), yp)
    clear_if(at_first("gy"), ym)


def behind_row(st, wz, k, x, y):
    if k in WZ_AT:
        return wz[WZ_AT[k], x, pl.ds(y, 1), :]
    return st[k, x, pl.ds(y, 1), :]


def wide(row):
    return jnp.broadcast_to(row, (8, 128))


def plane(x, first, last, fields, st, wz, acc_ref, at, diag_of):
    cache = {}

    def v(s, dx, y):
        key = (s, dx, y)
        if key not in cache:
            cache[key] = fields[SHIFT_AT[s]][x + dx, y]
        return cache[key]

    coef = {}

    def ahead(k, y):
        if OFF[k][2] == 0:
            if (k, 0, y) not in coef:
                coef[k, 0, y] = wide(st[k, x, pl.ds(y, 1), :])
            return coef[k, 0, y]
        return wide(st[k, x, pl.ds(y, 1), :])

    def behind(k, a, y):
        if k not in WZ_AT:
            if (k, a, y) not in coef:
                coef[k, a, y] = wide(st[k, x - a, pl.ds(y, 1), :])
            return coef[k, a, y]
        return wide(wz[WZ_AT[k], x - a, pl.ds(y, 1), :])

    for y in range(Y):
        parts = [None, None]
        n = 0
        for k, (a, b, c) in OFF.items():
            if 0 <= y + b < Y and not (a == 1 and last):
                term = ahead(k, y) * v(c, a, y + b)
                parts[n % 2] = term if parts[n % 2] is None else parts[n % 2] + term
                n += 1
            if 0 <= y - b < Y and not (a == 1 and first):
                term = behind(k, a, y - b) * v(-c, -a, y - b)
                parts[n % 2] = term if parts[n % 2] is None else parts[n % 2] + term
                n += 1
        acc_ref[at, y] = wide(diag_of(x, y, first)) * v(0, 0, y) - (parts[0] + parts[1])


def interior(fields, st, wz, acc_ref, diag_of):
    plane(0, True, False, fields, st, wz, acc_ref, 0, diag_of)

    def step(x, carry):
        plane(x, False, False, fields, st, wz, acc_ref, x, diag_of)
        return carry

    lax.fori_loop(1, X - 1, step, 0)
    plane(X - 1, False, True, fields, st, wz, acc_ref, X - 1, diag_of)


def inner_kernel(vi, vm, vp, st, wz, sums, acc, diag):
    def diag_of(x, y, first):
        total = sums[4, x, pl.ds(y, 1), :]
        if y > 0:
            total = total + sums[0, x, pl.ds(y - 1, 1), :]
        if not first:
            total = total + sums[2, x - 1, pl.ds(y, 1), :]
            if y > 0:
                total = total + sums[3, x - 1, pl.ds(y - 1, 1), :]
            if y < Y - 1:
                total = total + sums[1, x - 1, pl.ds(y + 1, 1), :]
        diag[x, pl.ds(y, 1), :] = total
        return total

    interior((vi, vm, vp), st, wz, acc, diag_of)


def inner_again_kernel(vi, vm, vp, st, wz, diag, acc):
    interior((vi, vm, vp), st, wz, acc, lambda x, y, first: diag[x, pl.ds(y, 1), :])


def ring_row(ref, keys, k, x):
    r = 16 * keys.index(k) + x
    return ref[24 + r // 8, pl.ds(r % 8, 1), :]


def third_kernel(with_diag):
    def body(*refs):
        if with_diag:
            vi, vm, vp, st, wz, rl, rr, qm, qp, sums, ring, xm, xp = refs
            qmw, qpw = qm, qp
        else:
            vi, vm, vp, st, wz, rl, rr, qm, qp, qmw, qpw, ring, xm, xp = refs
        for side, q, y in ((0, qm, Y - 1), (1, qp, 0)):
            for x in range(X):
                g = 16 + 2 * (x // 4)
                before, after = with_ends(q[x], ends_of((q[g], q[g + 1]), spot(x, y)))
                ring[side, 0, x] = q[x]
                ring[side, 1, x] = before
                ring[side, 2, x] = after
        xm[0] = qm[0]
        for y in range(Y):
            xm[1 + y] = vi[0, y]
        xm[Y + 1] = qp[0]
        for i, tile in enumerate((*merged(rl, rr, 0), qm[16], qm[17], qp[16], qp[17])):
            xm[Y + 2 + i] = tile
        last = X - 1
        for y in range(Y):
            total = None
            for k in XPLUS:
                _, b, c = OFF[k]
                s = SHIFT_AT[-c]
                if y - b < 0:
                    term = wide(ring_row(qmw, YPLUS, k, last)) * ring[0, s, last]
                elif y - b >= Y:
                    term = wide(ring_row(qpw, YMINUS, k, last)) * ring[1, s, last]
                else:
                    term = wide(behind_row(st, wz, k, last, y - b)) * (vi, vm, vp)[s][last, y - b]
                total = term if total is None else total + term
            xp[y] = total
            if with_diag:
                row = sums[2, last, pl.ds(y, 1), :]
                if y > 0:
                    row = row + sums[3, last, pl.ds(y - 1, 1), :]
                else:
                    for k in (11, 12, 13):
                        row = row + ring_row(qmw, YPLUS, k, last)
                if y < Y - 1:
                    row = row + sums[1, last, pl.ds(y + 1, 1), :]
                else:
                    for k in (5, 6, 7):
                        row = row + ring_row(qpw, YMINUS, k, last)
                xp[Y + y // 8, pl.ds(y % 8, 1), :] = row
        clear_if(at_first("gx"), xm)
        clear_if(at_last("gx"), xp)

    return body


def finish_edges(acc, st, ring, qmw, qpw, tp, tm, extra):
    last = X - 1
    far = {}

    def far_at(s, y):
        if (0, y) not in far:
            base, at = (Y + 2, y) if 0 <= y < Y else ((Y + 4, Y - 1) if y < 0 else (Y + 6, 0))
            far[0, y] = tp[y + 1]
            far[-1, y], far[1, y] = with_ends(tp[y + 1], ends_of((tp[base], tp[base + 1]), at))
        return far[s, y]

    for x in range(X):
        for y in range(Y) if x in (0, last) else (0, Y - 1):
            total = None
            for k, (a, b, c) in OFF.items():
                terms = []
                if x + a == X:
                    terms.append(wide(st[k, x, pl.ds(y, 1), :]) * far_at(c, y + b))
                elif y + b < 0:
                    terms.append(wide(st[k, x, pl.ds(y, 1), :]) * ring[0, SHIFT_AT[c], x + a])
                elif y + b >= Y:
                    terms.append(wide(st[k, x, pl.ds(y, 1), :]) * ring[1, SHIFT_AT[c], x + a])
                if x - a >= 0:
                    if y - b < 0:
                        terms.append(
                            wide(ring_row(qmw, YPLUS, k, x - a)) * ring[0, SHIFT_AT[-c], x - a]
                        )
                    elif y - b >= Y:
                        terms.append(
                            wide(ring_row(qpw, YMINUS, k, x - a)) * ring[1, SHIFT_AT[-c], x - a]
                        )
                for term in terms:
                    total = term if total is None else total + term
            if x == 0 and tm is not None:
                total = tm[y] if total is None else total + tm[y]
            if total is None:
                continue
            value = acc[x, y] - total
            fix = extra(x, y) if extra is not None else None
            acc[x, y] = value if fix is None else value + fix


def join_kernel(acc_in, diag_in, vi, st, ring, qm, qp, tp, tm, acc, diag, zp, zm):
    def fix(x, y):
        row = None
        if y == 0:
            for k in (2, 3, 4):
                r = ring_row(qm, YPLUS, k, x)
                row = r if row is None else row + r
            if x > 0:
                for k in (11, 12, 13):
                    row = row + ring_row(qm, YPLUS, k, x - 1)
        if y == Y - 1 and x > 0:
            for k in (5, 6, 7):
                r = ring_row(qp, YMINUS, k, x - 1)
                row = r if row is None else row + r
        if x == 0:
            r = tm[Y + y // 8, pl.ds(y % 8, 1), :]
            row = r if row is None else row + r
        if row is None:
            return None
        diag[x, pl.ds(y, 1), :] = diag[x, pl.ds(y, 1), :] + row
        return wide(row) * vi[x, y]

    finish_edges(acc, st, ring, qm, qp, tp, tm, fix)
    pack_columns(acc, zp, zm)
    clear_if(at_last("gz"), zp)
    clear_if(at_first("gz"), zm)


def turn_flat(v, out, x):
    for yb in range(4):
        out[:, x, pl.ds(8 * yb, 8), :] = jnp.swapaxes(v[x, pl.ds(8 * yb, 8)], 0, 1)


def flat_kernel(v, out):
    def turn(x, carry):
        turn_flat(v, out, x)
        return carry

    lax.fori_loop(0, X, turn, 0)


PRODUCTS = [(i, j) for i in range(8) for j in range(i, 8)]


def gram(u, v, planes=X, begin=None):
    def step(x, carry):
        for yb in range(4):
            at = pl.ds(8 * yb, 8)
            a = [u[i, x, at, :] for i in range(8)]
            b = a if v is u else [v[i, x, at, :] for i in range(8)]
            carry = tuple(c + a[i] * b[j] for c, (i, j) in zip(carry, PRODUCTS))
        return carry

    if begin is None:
        begin = tuple(jnp.zeros((8, 128), F32) for _ in PRODUCTS)
    return lax.fori_loop(0, planes, step, begin)


def place(tile, sums, m):
    held = dict(zip(PRODUCTS, sums))
    held = {p: jnp.sum(s, axis=1, keepdims=True) for p, s in held.items()}
    for i in range(8):
        row = jnp.zeros((8, 128), F32)
        for j in range(8):
            row = jnp.where(lanes() == 8 * m + j, held[min(i, j), max(i, j)], row)
        row = jnp.broadcast_to(jnp.sum(row, axis=0, keepdims=True), (8, 128))
        mine = (rows() == i) & (lanes() >= 8 * m) & (lanes() < 8 * m + 8)
        tile = jnp.where(mine, row, tile)
    return tile


def gram_first_kernel(r0, out):
    out[...] = place(jnp.zeros((8, 128), F32), gram(r0, r0), 0)


def gram_second_kernel(r0, y1, early, flat, out):
    flat_kernel(y1, flat)
    tile = place(early[...], gram(r0, flat), 1)
    out[...] = place(tile, gram(flat, flat), 2)


def late_kernel(acc_in, st, ring, qm, qp, tp, xp, y1, early, acc, flat, out, far, sent):
    finish_edges(acc, st, ring, qm, qp, tp, None, None)
    for yb in range(4):
        at = pl.ds(8 * yb, 8)
        far[:, 0, at, :] = jnp.swapaxes(tp[pl.ds(8 * yb + 1, 8)], 0, 1)
        sent[:, 0, at, :] = -jnp.swapaxes(xp[at], 0, 1)
    flat_kernel(acc, flat)
    sums = gram(far, sent, 1)
    out[...] = place(early[...], gram(y1, flat, X, sums), 3)


def differences_kernel(r0, y1, y2, tm, d0, d1):
    def step(x, carry):
        for i in range(8):
            d0[i, x] = r0[i, x] - y1[i, x]
            d1[i, x] = y1[i, x] - y2[i, x]
        return carry

    lax.fori_loop(0, X, step, 0)
    for yb in range(4):
        at = pl.ds(8 * yb, 8)
        d1[:, 0, at, :] = d1[:, 0, at, :] + jnp.swapaxes(tm[at], 0, 1)


def entry(col, i):
    return jnp.broadcast_to(col[i : i + 1, :], (8, 128))


def times(left, right):
    result = []
    for j in range(8):
        total = None
        for k in range(8):
            term = left[k] * entry(right[j], k)
            total = term if total is None else total + term
        result.append(total)
    return result


def flip(m):
    result = []
    for j in range(8):
        out = entry(m[0], j)
        for i in range(1, 8):
            out = jnp.where(rows() == i, entry(m[i], j), out)
        result.append(out)
    return result


def plus(left, right):
    return [a + b for a, b in zip(left, right)]


def minus(left, right):
    return [a - b for a, b in zip(left, right)]


def solve(matrix, right):
    a = list(matrix)
    r = list(right)
    for k in range(8):
        inverse = 1.0 / entry(a[k], k)
        here = rows() == k
        for cols, js in ((a, range(k + 1, 8)), (r, range(8))):
            for j in js:
                f = entry(cols[j], k) * inverse
                cols[j] = jnp.where(here, f, cols[j] - a[k] * f)
    return r


def moments(tile, m):
    return [jnp.broadcast_to(tile[:, 8 * m + j : 8 * m + j + 1], (8, 128)) for j in range(8)]


def coefficients(tile):
    m0, m1, m2, m3 = (moments(tile, m) for m in range(4))
    eye = [jnp.where(rows() == j, 1.0, 0.0) for j in range(8)]
    alpha = solve(m1, m0)
    inverse = solve(m0, eye)
    alpha_t = flip(alpha)
    m2a = times(m2, alpha)
    first = times(m1, alpha)
    rr1 = plus(minus(minus(m0, first), flip(first)), times(alpha_t, m2a))
    big = plus(eye, times(inverse, rr1))
    pq = plus(
        times(flip(big), minus(times(m1, big), m2a)),
        times(alpha_t, minus(times(m3, alpha), times(m2, big))),
    )
    alpha2 = solve(pq, rr1)
    return plus(alpha, times(big, alpha2)), times(alpha, alpha2)


def last_kernel(tile_ref, r0, y1, d0, d1, sol, res, coef, sbuf, rbuf, sems):
    c1, c2 = coefficients(tile_ref[...])
    for j in range(8):
        coef[0, j] = c1[j]
        coef[1, j] = c1[j] - c2[j]
        coef[2, j] = c2[j]

    def tile_out(x, yb):
        at = pl.ds(8 * yb, 8)
        a = [d0[i, x, at, :] for i in range(8)]
        b = [y1[i, x, at, :] for i in range(8)]
        c = [d1[i, x, at, :] for i in range(8)]
        for j in range(8):
            sums = []
            for m, field in enumerate((a, b, c)):
                total = None
                for i in range(8):
                    term = wide(coef[m, j, pl.ds(i, 1), :]) * field[i]
                    total = term if total is None else total + term
                sums.append(total)
            sbuf[j, x, at, :] = sums[0] + sums[1]
            rbuf[j, x, at, :] = r0[j, x, at, :] - (sums[1] + sums[2])

    def copy(n, src, dst, which):
        return pltpu.make_async_copy(src.at[:, n], dst.at[:, n], sems.at[which, n])

    def step(n, carry):
        for yb in range(4):
            tile_out(n, yb)
        copy(n, sbuf, sol, 0).start()
        copy(n, rbuf, res, 1).start()
        return carry

    lax.fori_loop(0, X, step, 0)
    for n in range(X):
        copy(n, sbuf, sol, 0).wait()
        copy(n, rbuf, res, 1).wait()


def shift(x, axis, step):
    n = lax.axis_size(axis)
    return lax.ppermute(x, axis, [(i, (i + step) % n) for i in range(n)])


def everywhere(x):
    for axis, bits in (("gy", (1, 2, 6)), ("gx", (1, 3)), ("gz", (1, 3))):
        n = lax.axis_size(axis)
        for bit in bits:
            x = x + lax.ppermute(x, axis, [(i, i ^ bit) for i in range(n)])
    return x


def shards(rhs, stencil):
    full = (X, Y, F, Z)
    compact = (F, X, Y, Z)
    tile = (8, 128)
    dma = pltpu.SemaphoreType.DMA
    st = stencil
    rc, vi, zp, zm = call(
        start_kernel, "k_start", [rhs, stencil],
        [compact, full, (9, *tile), (9, *tile)],
        in_specs=[FAR] * 2,
        scratch=[pltpu.VMEM((9, X, Y, Z), F32), dma((4,)), dma((9,))],
        limit=START_LIMIT,
    )
    rl = shift(zp, "gz", 1)
    rr = shift(zm, "gz", -1)
    vm, vp, wz = call(roll_kernel, "k_roll", [vi, st], [full, full, (9, X, Y, Z)])
    yp, ym = call(edge_kernel, "k_edge", [vi, st, wz, rl, rr], [(36, *tile), (30, *tile)])
    qm = shift(yp, "gy", 1)
    qp = shift(ym, "gy", -1)
    vm, vp, wz, sums = call(
        ends_kernel, "k_ends", [vm, vp, wz, st, rl, rr],
        [full, full, (9, X, Y, Z), (5, X, Y, Z)], aliases={0: 0, 1: 1, 2: 2}, after=[yp],
    )
    (g0,) = call(gram_first_kernel, "k_gram0", [rc], [tile], after=[yp])
    ring, xm, xp = call(
        third_kernel(True), "k_third", [vi, vm, vp, st, wz, rl, rr, qm, qp, sums],
        [(2, 3, X, *tile), (Y + 8, *tile), (Y + 4, *tile)], after=[g0],
    )
    tp = shift(xm, "gx", -1)
    tm = shift(xp, "gx", 1)
    acc, diag = call(inner_kernel, "k_inner", [vi, vm, vp, st, wz, sums], [full, (X, Y, Z)])
    y1, diag, zp, zm = call(
        join_kernel, "k_join", [acc, diag, vi, st, ring, qm, qp, tp, tm],
        [full, (X, Y, Z), (4, *tile), (4, *tile)], aliases={0: 0, 1: 1},
    )

    rl = shift(zp, "gz", 1)
    rr = shift(zm, "gz", -1)
    vm, vp = call(roll_fields, "k_roll2", [y1], [full, full])
    yp, ym = call(
        edge_again_kernel, "k_edge2", [y1, rl, rr], [(24, *tile), (24, *tile)], after=[vm]
    )
    qmv = shift(yp, "gy", 1)
    qpv = shift(ym, "gy", -1)
    vm, vp = call(
        ends_again_kernel, "k_ends2", [vm, vp, rl, rr], [full, full],
        aliases={0: 0, 1: 1}, after=[yp],
    )
    y1f, g2 = call(gram_second_kernel, "k_gram12", [rc, y1, g0], [compact, tile], after=[yp])
    ring, xm, xp = call(
        third_kernel(False), "k_third2", [y1, vm, vp, st, wz, rl, rr, qmv, qpv, qm, qp],
        [(2, 3, X, *tile), (Y + 8, *tile), (Y, *tile)], after=[g2],
    )
    tp = shift(xm, "gx", -1)
    tm = shift(xp, "gx", 1)
    (acc,) = call(inner_again_kernel, "k_inner2", [y1, vm, vp, st, wz, diag], [full])
    _, y2f, moment = call(
        late_kernel, "k_late", [acc, st, ring, qm, qp, tp, xp, y1f, g2],
        [full, compact, tile], aliases={0: 0},
        scratch=[pltpu.VMEM((F, 1, Y, Z), F32), pltpu.VMEM((F, 1, Y, Z), F32)],
    )
    d0, d1 = call(differences_kernel, "k_diff", [rc, y1f, y2f, tm], [compact, compact])
    moment = everywhere(moment)
    sol, res = call(
        last_kernel, "k_last", [moment, rc, y1f, d0, d1], [compact, compact],
        out_specs=[FAR, FAR],
        scratch=[
            pltpu.VMEM((3, 8, *tile), F32),
            pltpu.VMEM(compact, F32),
            pltpu.VMEM(compact, F32),
            dma((2, X)),
        ],
        limit=14,
    )
    return sol, res


def solution(mesh):
    placed = P(None, "gx", "gy", "gz")
    return jax.shard_map(
        shards, mesh=mesh, in_specs=(placed, placed), out_specs=(placed, placed), check_vma=False
    )
```

```python
import jax
import jax.numpy as jnp
from jax import lax
from jax.experimental import pallas as pl
from jax.experimental.pallas import tpu as pltpu
from jax.sharding import PartitionSpec as P

F32 = jnp.float32
X, Y, Z, F = 16, 32, 128, 8
FORWARD = [
    (a, b, c) for a in (-1, 0, 1) for b in (-1, 0, 1) for c in (-1, 0, 1) if (a, b, c) > (0, 0, 0)
]
OFF = {k + 1: o for k, o in enumerate(FORWARD)}
ZPLUS = [k for k in OFF if OFF[k][2] == 1]
ZMINUS = [k for k in OFF if OFF[k][2] == -1]
YPLUS = [k for k in OFF if OFF[k][1] == 1]
YMINUS = [k for k in OFF if OFF[k][1] == -1]
XPLUS = [k for k in OFF if OFF[k][0] == 1]
ZSHIFTED = ZPLUS + ZMINUS
WZ_AT = {k: i for i, k in enumerate(ZSHIFTED)}
PAIRS = tuple(zip(ZPLUS, ZMINUS + [None]))
GROUPS = ((0, 1), (1, -1), (1, 0), (1, 1))
SHIFT_AT = {0: 0, -1: 1, 1: 2}

VSPEC = pl.BlockSpec(memory_space=pltpu.VMEM)
HSPEC = pl.BlockSpec(memory_space=pl.ANY)
FAR = pl.BlockSpec(memory_space=pltpu.HBM)
MIB = 1024 * 1024
START_LIMIT = 48


def call(body, name, ins, outs, after=(), aliases=None, scratch=(), in_specs=None, out_specs=None, limit=8):
    count = len(ins)

    def run(*refs):
        body(*refs[:count], *refs[count + len(after):])

    return pl.pallas_call(
        run,
        name=name,
        out_shape=[jax.ShapeDtypeStruct(s, F32) for s in outs],
        in_specs=(in_specs or [VSPEC] * count) + [HSPEC] * len(after),
        out_specs=out_specs or [VSPEC] * len(outs),
        input_output_aliases=aliases or {},
        scratch_shapes=list(scratch),
        compiler_params=pltpu.CompilerParams(vmem_limit_bytes=limit * MIB),
    )(*ins, *after)


def lanes():
    return lax.broadcasted_iota(jnp.int32, (8, 128), 1)


def rows():
    return lax.broadcasted_iota(jnp.int32, (8, 128), 0)


def roll(v, shift):
    shift %= 128
    return pltpu.roll(v, shift, axis=1) if shift else v


def spot(x, y):
    return (x % 4) * 32 + y


def with_ends(value, ends):
    before = jnp.where(lanes() == 0, ends, roll(value, 1))
    after = jnp.where(lanes() == 127, ends, roll(value, -1))
    return before, after


def clear_if(condition, *outs):
    @pl.when(condition)
    def _():
        for ref in outs:
            ref[...] = jnp.zeros(ref.shape, F32)


def at_first(axis):
    return lax.axis_index(axis) == 0


def at_last(axis):
    return lax.axis_index(axis) == lax.axis_size(axis) - 1


def pack_group(field, g, zp, zm):
    high = jnp.zeros((8, 128), F32)
    low = jnp.zeros((8, 128), F32)
    for xx in range(4):
        for y in range(Y):
            at = spot(xx, y)
            v = roll(field[4 * g + xx, y], at + 1)
            high = jnp.where(lanes() == at, v, high)
            low = jnp.where(lanes() == (at + 1) % 128, v, low)
    zp[g] = high
    zm[g] = low


def pack_columns(field, zp, zm):
    def group(g, carry):
        pack_group(field, g, zp, zm)
        return carry

    lax.fori_loop(0, 4, group, 0)


def start_kernel(rhs, stencil, rc, vi, zp, zm, st, sem_r, sem_s):
    def part(g):
        at = pl.ds(4 * g, 4)
        return pltpu.make_async_copy(rhs.at[:, at], rc.at[:, at], sem_r.at[g])

    def field(k):
        at = WZ_AT[k]
        return pltpu.make_async_copy(stencil.at[k], st.at[at], sem_s.at[at])

    order = [k for pair in PAIRS for k in pair if k is not None]
    for g in range(4):
        part(g).start()
    for k in order:
        field(k).start()

    def group(g, carry):
        part(g).wait()
        for xx in range(4):
            x = 4 * g + xx
            for yb in range(4):
                vi[x, pl.ds(8 * yb, 8)] = jnp.swapaxes(rc[:, x, pl.ds(8 * yb, 8), :], 0, 1)
        pack_group(vi, g, zp, zm)
        return carry

    lax.fori_loop(0, 4, group, 0)
    for k in order:
        field(k).wait()
    for j, (up, down) in enumerate(PAIRS):
        out = jnp.zeros((8, 128), F32)
        for x in range(X):
            for yb in range(4):
                at = 8 * x + 2 * yb
                w = st[WZ_AT[up], x, pl.ds(8 * yb, 8), :]
                if down is not None:
                    w = jnp.where(lanes() == 0, st[WZ_AT[down], x, pl.ds(8 * yb, 8), :], w)
                out = jnp.where((lanes() == at) | (lanes() == at + 1), roll(w, at + 1), out)
        zp[4 + j] = out
        zm[4 + j] = out
    clear_if(at_last("gz"), zp)
    clear_if(at_first("gz"), zm)


def even():
    return (lanes() & 1) == 0


def merged(rl, rr, g):
    left, right = roll(rl[g], 2), rr[g]
    return jnp.where(even(), left, right), jnp.where(even(), right, left)


def ends_of(pair, at):
    return roll(pair[at % 2], -(at + 2))


def coupling_ends(rl, rr):
    return [jnp.where(even(), roll(rl[4 + j], 2), rr[4 + j]) for j in range(5)]


def coupling_end(ends, j, x, yb):
    return roll(ends[j], -(8 * x + 2 * yb + 2))


def roll_rows(vi, vm, vp, x):
    for y in range(Y):
        v = vi[x, y]
        vm[x, y] = roll(v, 1)
        vp[x, y] = roll(v, -1)


def roll_fields(vi, vm, vp):
    def step(n, carry):
        for i in range(4):
            roll_rows(vi, vm, vp, 4 * n + i)
        return carry

    lax.fori_loop(0, X // 4, step, 0)


def roll_kernel(vi, st, vm, vp, wz):
    def step(n, carry):
        for i in range(4):
            x = 4 * n + i
            roll_rows(vi, vm, vp, x)
            for k in ZSHIFTED:
                for yb in range(4):
                    at = pl.ds(8 * yb, 8)
                    wz[WZ_AT[k], x, at, :] = roll(st[k, x, at, :], OFF[k][2])
        return carry

    lax.fori_loop(0, X // 4, step, 0)


def put_ends(rl, rr, vm, vp):
    first, last = lanes() == 0, lanes() == 127

    def group(g, carry):
        pair = merged(rl, rr, g)
        for xx in range(4):
            for y in range(Y):
                end = ends_of(pair, spot(xx, y))
                pltpu.store(vm.at[4 * g + xx, y], end, mask=first)
                pltpu.store(vp.at[4 * g + xx, y], end, mask=last)
        return carry

    lax.fori_loop(0, 4, group, 0)


def ends_kernel(vm_in, vp_in, wz_in, st, rl, rr, vm, vp, wz, sums):
    put_ends(rl, rr, vm, vp)
    ends = coupling_ends(rl, rr)
    first, last = lanes() == 0, lanes() == 127
    for j, pair in enumerate(PAIRS):
        for x in range(X):
            for yb in range(4):
                end = coupling_end(ends, j, x, yb)
                for k, mask in zip(pair, (first, last)):
                    if k is not None:
                        pltpu.store(wz.at[WZ_AT[k], x, pl.ds(8 * yb, 8), :], end, mask=mask)

    def behind(k, x, yb):
        if k in WZ_AT:
            return wz[WZ_AT[k], x, pl.ds(8 * yb, 8), :]
        return st[k, x, pl.ds(8 * yb, 8), :]

    def add_up(x, carry):
        for yb in range(4):
            total = st[0, x, pl.ds(8 * yb, 8), :]
            for k in OFF:
                total = total + st[k, x, pl.ds(8 * yb, 8), :]
            sums[4, x, pl.ds(8 * yb, 8), :] = total + behind(1, x, yb)
            for i, (a, b) in enumerate(GROUPS):
                keys = [k for k in OFF if OFF[k][:2] == (a, b)]
                sums[i, x, pl.ds(8 * yb, 8), :] = (
                    behind(keys[0], x, yb) + behind(keys[1], x, yb) + behind(keys[2], x, yb)
                )
        return carry

    lax.fori_loop(0, X, add_up, 0)


def ends_again_kernel(vm_in, vp_in, rl, rr, vm, vp):
    put_ends(rl, rr, vm, vp)


def edge_rows(vi, rl, rr, yp, ym):
    for x in range(X):
        yp[x] = vi[x, Y - 1]
        ym[x] = vi[x, 0]
    for g in range(4):
        for i, tile in enumerate(merged(rl, rr, g)):
            yp[16 + 2 * g + i] = tile
            ym[16 + 2 * g + i] = tile


def edge_kernel(vi, st, wz, rl, rr, yp, ym):
    edge_rows(vi, rl, rr, yp, ym)
    ends = coupling_ends(rl, rr)
    for ref, keys, y in ((yp, YPLUS, Y - 1), (ym, YMINUS, 0)):
        rows_of = {}
        for j, pair in enumerate(PAIRS):
            for x in range(X):
                for k, edge in zip(pair, (0, 127)):
                    if k in keys:
                        end = coupling_end(ends, j, x, y // 8)
                        w = wz[WZ_AT[k], x, pl.ds(8 * (y // 8), 8), :]
                        rows_of[k, x] = jnp.where(lanes() == edge, end, w)
        for i, k in enumerate(keys):
            for x in range(X):
                r = 16 * i + x
                if k in WZ_AT:
                    row = rows_of[k, x][y % 8 : y % 8 + 1, :]
                else:
                    row = st[k, x, pl.ds(y, 1), :]
                ref[24 + r // 8, pl.ds(r % 8, 1), :] = row
    clear_if(at_last("gy"), yp)
    clear_if(at_first("gy"), ym)


def edge_again_kernel(vi, rl, rr, yp, ym):
    edge_rows(vi, rl, rr, yp, ym)
    clear_if(at_last("gy"), yp)
    clear_if(at_first("gy"), ym)


def behind_row(st, wz, k, x, y):
    if k in WZ_AT:
        return wz[WZ_AT[k], x, pl.ds(y, 1), :]
    return st[k, x, pl.ds(y, 1), :]


def wide(row):
    return jnp.broadcast_to(row, (8, 128))


def plane(x, first, last, fields, st, wz, acc_ref, at, diag_of):
    cache = {}

    def v(s, dx, y):
        key = (s, dx, y)
        if key not in cache:
            cache[key] = fields[SHIFT_AT[s]][x + dx, y]
        return cache[key]

    coef = {}

    def ahead(k, y):
        if OFF[k][2] == 0:
            if (k, 0, y) not in coef:
                coef[k, 0, y] = wide(st[k, x, pl.ds(y, 1), :])
            return coef[k, 0, y]
        return wide(st[k, x, pl.ds(y, 1), :])

    def behind(k, a, y):
        if k not in WZ_AT:
            if (k, a, y) not in coef:
                coef[k, a, y] = wide(st[k, x - a, pl.ds(y, 1), :])
            return coef[k, a, y]
        return wide(wz[WZ_AT[k], x - a, pl.ds(y, 1), :])

    for y in range(Y):
        parts = [None, None]
        n = 0
        for k, (a, b, c) in OFF.items():
            if 0 <= y + b < Y and not (a == 1 and last):
                term = ahead(k, y) * v(c, a, y + b)
                parts[n % 2] = term if parts[n % 2] is None else parts[n % 2] + term
                n += 1
            if 0 <= y - b < Y and not (a == 1 and first):
                term = behind(k, a, y - b) * v(-c, -a, y - b)
                parts[n % 2] = term if parts[n % 2] is None else parts[n % 2] + term
                n += 1
        acc_ref[at, y] = wide(diag_of(x, y, first)) * v(0, 0, y) - (parts[0] + parts[1])


def interior(fields, st, wz, acc_ref, diag_of):
    plane(0, True, False, fields, st, wz, acc_ref, 0, diag_of)

    def step(x, carry):
        plane(x, False, False, fields, st, wz, acc_ref, x, diag_of)
        return carry

    lax.fori_loop(1, X - 1, step, 0)
    plane(X - 1, False, True, fields, st, wz, acc_ref, X - 1, diag_of)


def inner_kernel(vi, vm, vp, st, wz, sums, acc, diag):
    def diag_of(x, y, first):
        total = sums[4, x, pl.ds(y, 1), :]
        if y > 0:
            total = total + sums[0, x, pl.ds(y - 1, 1), :]
        if not first:
            total = total + sums[2, x - 1, pl.ds(y, 1), :]
            if y > 0:
                total = total + sums[3, x - 1, pl.ds(y - 1, 1), :]
            if y < Y - 1:
                total = total + sums[1, x - 1, pl.ds(y + 1, 1), :]
        diag[x, pl.ds(y, 1), :] = total
        return total

    interior((vi, vm, vp), st, wz, acc, diag_of)


def inner_again_kernel(vi, vm, vp, st, wz, diag, xp, acc, sent):
    sent[...] = xp[...]
    interior((vi, vm, vp), st, wz, acc, lambda x, y, first: diag[x, pl.ds(y, 1), :])


def ring_row(ref, keys, k, x):
    r = 16 * keys.index(k) + x
    return ref[24 + r // 8, pl.ds(r % 8, 1), :]


def third_kernel(with_diag):
    def body(*refs):
        if with_diag:
            vi, vm, vp, st, wz, rl, rr, qm, qp, sums, ring, xm, xp = refs
            qmw, qpw = qm, qp
        else:
            vi, vm, vp, st, wz, rl, rr, qm, qp, qmw, qpw, ring, xm, xp = refs
        for side, q, y in ((0, qm, Y - 1), (1, qp, 0)):
            for x in range(X):
                g = 16 + 2 * (x // 4)
                before, after = with_ends(q[x], ends_of((q[g], q[g + 1]), spot(x, y)))
                ring[side, 0, x] = q[x]
                ring[side, 1, x] = before
                ring[side, 2, x] = after
        xm[0] = qm[0]
        for y in range(Y):
            xm[1 + y] = vi[0, y]
        xm[Y + 1] = qp[0]
        for i, tile in enumerate((*merged(rl, rr, 0), qm[16], qm[17], qp[16], qp[17])):
            xm[Y + 2 + i] = tile
        last = X - 1
        for y in range(Y):
            total = None
            for k in XPLUS:
                _, b, c = OFF[k]
                s = SHIFT_AT[-c]
                if y - b < 0:
                    term = wide(ring_row(qmw, YPLUS, k, last)) * ring[0, s, last]
                elif y - b >= Y:
                    term = wide(ring_row(qpw, YMINUS, k, last)) * ring[1, s, last]
                else:
                    term = wide(behind_row(st, wz, k, last, y - b)) * (vi, vm, vp)[s][last, y - b]
                total = term if total is None else total + term
            xp[y] = total
            if with_diag:
                row = sums[2, last, pl.ds(y, 1), :]
                if y > 0:
                    row = row + sums[3, last, pl.ds(y - 1, 1), :]
                else:
                    for k in (11, 12, 13):
                        row = row + ring_row(qmw, YPLUS, k, last)
                if y < Y - 1:
                    row = row + sums[1, last, pl.ds(y + 1, 1), :]
                else:
                    for k in (5, 6, 7):
                        row = row + ring_row(qpw, YMINUS, k, last)
                xp[Y + y // 8, pl.ds(y % 8, 1), :] = row
        clear_if(at_first("gx"), xm)
        clear_if(at_last("gx"), xp)

    return body


def finish_edges(acc, st, ring, qmw, qpw, tp, tm, extra):
    last = X - 1
    far = {}

    def far_at(s, y):
        if (0, y) not in far:
            base, at = (Y + 2, y) if 0 <= y < Y else ((Y + 4, Y - 1) if y < 0 else (Y + 6, 0))
            far[0, y] = tp[y + 1]
            far[-1, y], far[1, y] = with_ends(tp[y + 1], ends_of((tp[base], tp[base + 1]), at))
        return far[s, y]

    for x in range(X):
        for y in range(Y) if x in (0, last) else (0, Y - 1):
            total = None
            for k, (a, b, c) in OFF.items():
                terms = []
                if x + a == X:
                    terms.append(wide(st[k, x, pl.ds(y, 1), :]) * far_at(c, y + b))
                elif y + b < 0:
                    terms.append(wide(st[k, x, pl.ds(y, 1), :]) * ring[0, SHIFT_AT[c], x + a])
                elif y + b >= Y:
                    terms.append(wide(st[k, x, pl.ds(y, 1), :]) * ring[1, SHIFT_AT[c], x + a])
                if x - a >= 0:
                    if y - b < 0:
                        terms.append(
                            wide(ring_row(qmw, YPLUS, k, x - a)) * ring[0, SHIFT_AT[-c], x - a]
                        )
                    elif y - b >= Y:
                        terms.append(
                            wide(ring_row(qpw, YMINUS, k, x - a)) * ring[1, SHIFT_AT[-c], x - a]
                        )
                for term in terms:
                    total = term if total is None else total + term
            if x == 0 and tm is not None:
                total = tm[y] if total is None else total + tm[y]
            if total is None:
                continue
            value = acc[x, y] - total
            fix = extra(x, y) if extra is not None else None
            acc[x, y] = value if fix is None else value + fix


def join_kernel(acc_in, diag_in, vi, st, ring, qm, qp, tp, tm, acc, diag, zp, zm):
    def fix(x, y):
        row = None
        if y == 0:
            for k in (2, 3, 4):
                r = ring_row(qm, YPLUS, k, x)
                row = r if row is None else row + r
            if x > 0:
                for k in (11, 12, 13):
                    row = row + ring_row(qm, YPLUS, k, x - 1)
        if y == Y - 1 and x > 0:
            for k in (5, 6, 7):
                r = ring_row(qp, YMINUS, k, x - 1)
                row = r if row is None else row + r
        if x == 0:
            r = tm[Y + y // 8, pl.ds(y % 8, 1), :]
            row = r if row is None else row + r
        if row is None:
            return None
        diag[x, pl.ds(y, 1), :] = diag[x, pl.ds(y, 1), :] + row
        return wide(row) * vi[x, y]

    finish_edges(acc, st, ring, qm, qp, tp, tm, fix)
    pack_columns(acc, zp, zm)
    clear_if(at_last("gz"), zp)
    clear_if(at_first("gz"), zm)


def turn_flat(v, out, x):
    for yb in range(4):
        out[:, x, pl.ds(8 * yb, 8), :] = jnp.swapaxes(v[x, pl.ds(8 * yb, 8)], 0, 1)


def flat_kernel(v, out):
    def turn(x, carry):
        turn_flat(v, out, x)
        return carry

    lax.fori_loop(0, X, turn, 0)


PRODUCTS = [(i, j) for i in range(8) for j in range(i, 8)]


def gram(u, v, planes=X, begin=None):
    def step(x, carry):
        for yb in range(4):
            at = pl.ds(8 * yb, 8)
            a = [u[i, x, at, :] for i in range(8)]
            b = a if v is u else [v[i, x, at, :] for i in range(8)]
            carry = tuple(c + a[i] * b[j] for c, (i, j) in zip(carry, PRODUCTS))
        return carry

    if begin is None:
        begin = tuple(jnp.zeros((8, 128), F32) for _ in PRODUCTS)
    return lax.fori_loop(0, planes, step, begin)


def place(tile, sums, m):
    held = dict(zip(PRODUCTS, sums))
    held = {p: jnp.sum(s, axis=1, keepdims=True) for p, s in held.items()}
    for i in range(8):
        row = jnp.zeros((8, 128), F32)
        for j in range(8):
            row = jnp.where(lanes() == 8 * m + j, held[min(i, j), max(i, j)], row)
        row = jnp.broadcast_to(jnp.sum(row, axis=0, keepdims=True), (8, 128))
        mine = (rows() == i) & (lanes() >= 8 * m) & (lanes() < 8 * m + 8)
        tile = jnp.where(mine, row, tile)
    return tile


def gram_first_kernel(r0, out):
    out[...] = place(jnp.zeros((8, 128), F32), gram(r0, r0), 0)


def gram_second_kernel(r0, y1, early, flat, out):
    flat_kernel(y1, flat)
    tile = place(early[...], gram(r0, flat), 1)
    out[...] = place(tile, gram(flat, flat), 2)


def late_kernel(acc_in, st, ring, qm, qp, tp, xp, y1, early, acc, flat, out, far, sent):
    finish_edges(acc, st, ring, qm, qp, tp, None, None)
    for yb in range(4):
        at = pl.ds(8 * yb, 8)
        far[:, 0, at, :] = jnp.swapaxes(tp[pl.ds(8 * yb + 1, 8)], 0, 1)
        sent[:, 0, at, :] = -jnp.swapaxes(xp[at], 0, 1)
    flat_kernel(acc, flat)
    sums = gram(far, sent, 1)
    out[...] = place(early[...], gram(y1, flat, X, sums), 3)


def differences_kernel(r0, y1, y2, tm, d0, d1):
    def step(x, carry):
        for i in range(8):
            d0[i, x] = r0[i, x] - y1[i, x]
            d1[i, x] = y1[i, x] - y2[i, x]
        return carry

    lax.fori_loop(0, X, step, 0)
    for yb in range(4):
        at = pl.ds(8 * yb, 8)
        d1[:, 0, at, :] = d1[:, 0, at, :] + jnp.swapaxes(tm[at], 0, 1)


def entry(col, i):
    return jnp.broadcast_to(col[i : i + 1, :], (8, 128))


def times(left, right):
    result = []
    for j in range(8):
        total = None
        for k in range(8):
            term = left[k] * entry(right[j], k)
            total = term if total is None else total + term
        result.append(total)
    return result


def flip(m):
    result = []
    for j in range(8):
        out = entry(m[0], j)
        for i in range(1, 8):
            out = jnp.where(rows() == i, entry(m[i], j), out)
        result.append(out)
    return result


def plus(left, right):
    return [a + b for a, b in zip(left, right)]


def minus(left, right):
    return [a - b for a, b in zip(left, right)]


def solve(matrix, right):
    a = list(matrix)
    r = list(right)
    for k in range(8):
        inverse = 1.0 / entry(a[k], k)
        here = rows() == k
        for cols, js in ((a, range(k + 1, 8)), (r, range(8))):
            for j in js:
                f = entry(cols[j], k) * inverse
                cols[j] = jnp.where(here, f, cols[j] - a[k] * f)
    return r


def moments(tile, m):
    return [jnp.broadcast_to(tile[:, 8 * m + j : 8 * m + j + 1], (8, 128)) for j in range(8)]


def coefficients(tile):
    m0, m1, m2, m3 = (moments(tile, m) for m in range(4))
    eye = [jnp.where(rows() == j, 1.0, 0.0) for j in range(8)]
    alpha = solve(m1, m0)
    inverse = solve(m0, eye)
    alpha_t = flip(alpha)
    m2a = times(m2, alpha)
    first = times(m1, alpha)
    rr1 = plus(minus(minus(m0, first), flip(first)), times(alpha_t, m2a))
    big = plus(eye, times(inverse, rr1))
    pq = plus(
        times(flip(big), minus(times(m1, big), m2a)),
        times(alpha_t, minus(times(m3, alpha), times(m2, big))),
    )
    alpha2 = solve(pq, rr1)
    return plus(alpha, times(big, alpha2)), times(alpha, alpha2)


def last_kernel(tile_ref, r0, y1, d0, d1, sol, res, coef, sbuf, rbuf, sems):
    c1, c2 = coefficients(tile_ref[...])
    for j in range(8):
        coef[0, j] = c1[j]
        coef[1, j] = c1[j] - c2[j]
        coef[2, j] = c2[j]

    def tile_out(x, yb):
        at = pl.ds(8 * yb, 8)
        a = [d0[i, x, at, :] for i in range(8)]
        b = [y1[i, x, at, :] for i in range(8)]
        c = [d1[i, x, at, :] for i in range(8)]
        for j in range(8):
            sums = []
            for m, field in enumerate((a, b, c)):
                total = None
                for i in range(8):
                    term = wide(coef[m, j, pl.ds(i, 1), :]) * field[i]
                    total = term if total is None else total + term
                sums.append(total)
            sbuf[j, x, at, :] = sums[0] + sums[1]
            rbuf[j, x, at, :] = r0[j, x, at, :] - (sums[1] + sums[2])

    def copy(n, src, dst, which):
        return pltpu.make_async_copy(src.at[:, n], dst.at[:, n], sems.at[which, n])

    def step(n, carry):
        for yb in range(4):
            tile_out(n, yb)
        copy(n, sbuf, sol, 0).start()
        copy(n, rbuf, res, 1).start()
        return carry

    lax.fori_loop(0, X, step, 0)
    for n in range(X):
        copy(n, sbuf, sol, 0).wait()
        copy(n, rbuf, res, 1).wait()


def shift(x, axis, step):
    n = lax.axis_size(axis)
    return lax.ppermute(x, axis, [(i, (i + step) % n) for i in range(n)])


def ring_sum(x, axis, stride):
    left, right, across = (shift(x, axis, n * stride) for n in (1, -1, 2))
    return (x + across) + (left + right)


def other_core(x):
    n = lax.axis_size("gy")
    return lax.ppermute(x, "gy", [(i, i ^ 1) for i in range(n)])


def shards(rhs, stencil):
    full = (X, Y, F, Z)
    compact = (F, X, Y, Z)
    tile = (8, 128)
    dma = pltpu.SemaphoreType.DMA
    st = stencil
    rc, vi, zp, zm = call(
        start_kernel, "k_start", [rhs, stencil],
        [compact, full, (9, *tile), (9, *tile)],
        in_specs=[FAR] * 2,
        scratch=[pltpu.VMEM((9, X, Y, Z), F32), dma((4,)), dma((9,))],
        limit=START_LIMIT,
    )
    rl = shift(zp, "gz", 1)
    rr = shift(zm, "gz", -1)
    vm, vp, wz = call(roll_kernel, "k_roll", [vi, st], [full, full, (9, X, Y, Z)])
    yp, ym = call(edge_kernel, "k_edge", [vi, st, wz, rl, rr], [(36, *tile), (30, *tile)])
    qm = shift(yp, "gy", 1)
    qp = shift(ym, "gy", -1)
    vm, vp, wz, sums = call(
        ends_kernel, "k_ends", [vm, vp, wz, st, rl, rr],
        [full, full, (9, X, Y, Z), (5, X, Y, Z)], aliases={0: 0, 1: 1, 2: 2}, after=[yp],
    )
    ring, xm, xp = call(
        third_kernel(True), "k_third", [vi, vm, vp, st, wz, rl, rr, qm, qp, sums],
        [(2, 3, X, *tile), (Y + 8, *tile), (Y + 4, *tile)],
    )
    tp = shift(xm, "gx", -1)
    tm = shift(xp, "gx", 1)
    acc, diag = call(inner_kernel, "k_inner", [vi, vm, vp, st, wz, sums], [full, (X, Y, Z)])
    y1, diag, zp, zm = call(
        join_kernel, "k_join", [acc, diag, vi, st, ring, qm, qp, tp, tm],
        [full, (X, Y, Z), (4, *tile), (4, *tile)], aliases={0: 0, 1: 1},
    )

    rl = shift(zp, "gz", 1)
    rr = shift(zm, "gz", -1)
    vm, vp = call(roll_fields, "k_roll2", [y1], [full, full])
    (g0,) = call(gram_first_kernel, "k_gram0", [rc], [tile], after=[zp])
    yp, ym = call(
        edge_again_kernel, "k_edge2", [y1, rl, rr], [(24, *tile), (24, *tile)], after=[vm, g0]
    )
    qmv = shift(yp, "gy", 1)
    qpv = shift(ym, "gy", -1)
    vm, vp = call(
        ends_again_kernel, "k_ends2", [vm, vp, rl, rr], [full, full],
        aliases={0: 0, 1: 1}, after=[yp],
    )
    y1f, g2 = call(gram_second_kernel, "k_gram12", [rc, y1, g0], [compact, tile], after=[yp])
    ring, xm, xp = call(
        third_kernel(False), "k_third2", [y1, vm, vp, st, wz, rl, rr, qmv, qpv, qm, qp],
        [(2, 3, X, *tile), (Y + 8, *tile), (Y, *tile)], after=[g2],
    )
    tp = shift(xm, "gx", -1)
    acc, xp = call(
        inner_again_kernel, "k_inner2", [y1, vm, vp, st, wz, diag, xp], [full, (Y, *tile)]
    )
    tm = shift(xp, "gx", 1)
    _, y2f, moment = call(
        late_kernel, "k_late", [acc, st, ring, qm, qp, tp, xp, y1f, g2],
        [full, compact, tile], aliases={0: 0},
        scratch=[pltpu.VMEM((F, 1, Y, Z), F32), pltpu.VMEM((F, 1, Y, Z), F32)],
    )
    d0, d1 = call(differences_kernel, "k_diff", [rc, y1f, y2f, tm], [compact, compact])
    moment = ring_sum(ring_sum(moment, "gx", 1), "gz", 1)
    moment = ring_sum(moment + other_core(moment), "gy", 2)
    sol, res = call(
        last_kernel, "k_last", [moment, rc, y1f, d0, d1], [compact, compact],
        out_specs=[FAR, FAR],
        scratch=[
            pltpu.VMEM((3, 8, *tile), F32),
            pltpu.VMEM(compact, F32),
            pltpu.VMEM(compact, F32),
            dma((2, X)),
        ],
        limit=14,
    )
    return sol, res


def solution(mesh):
    placed = P(None, "gx", "gy", "gz")
    return jax.shard_map(
        shards, mesh=mesh, in_specs=(placed, placed), out_specs=(placed, placed), check_vma=False
    )
```

```python
import jax
import jax.numpy as jnp
from jax import lax
from jax.experimental import pallas as pl
from jax.experimental.pallas import tpu as pltpu
from jax.sharding import PartitionSpec as P

F32 = jnp.float32
X, Y, Z, F = 16, 32, 128, 8
FORWARD = [
    (a, b, c) for a in (-1, 0, 1) for b in (-1, 0, 1) for c in (-1, 0, 1) if (a, b, c) > (0, 0, 0)
]
OFF = {k + 1: o for k, o in enumerate(FORWARD)}
ZPLUS = [k for k in OFF if OFF[k][2] == 1]
ZMINUS = [k for k in OFF if OFF[k][2] == -1]
YPLUS = [k for k in OFF if OFF[k][1] == 1]
YMINUS = [k for k in OFF if OFF[k][1] == -1]
XPLUS = [k for k in OFF if OFF[k][0] == 1]
ZSHIFTED = ZPLUS + ZMINUS
WZ_AT = {k: i for i, k in enumerate(ZSHIFTED)}
PAIRS = tuple(zip(ZPLUS, ZMINUS + [None]))
GROUPS = ((0, 1), (1, -1), (1, 0), (1, 1))
SHIFT_AT = {0: 0, -1: 1, 1: 2}

VSPEC = pl.BlockSpec(memory_space=pltpu.VMEM)
HSPEC = pl.BlockSpec(memory_space=pl.ANY)
FAR = pl.BlockSpec(memory_space=pltpu.HBM)
MIB = 1024 * 1024
START_LIMIT = 48


def call(body, ins, outs, after=(), aliases=None, scratch=(), in_specs=None, out_specs=None, limit=8):
    count = len(ins)

    def run(*refs):
        body(*refs[:count], *refs[count + len(after):])

    return pl.pallas_call(
        run,
        out_shape=[jax.ShapeDtypeStruct(s, F32) for s in outs],
        in_specs=(in_specs or [VSPEC] * count) + [HSPEC] * len(after),
        out_specs=out_specs or [VSPEC] * len(outs),
        input_output_aliases=aliases or {},
        scratch_shapes=list(scratch),
        compiler_params=pltpu.CompilerParams(vmem_limit_bytes=limit * MIB),
    )(*ins, *after)


def lanes():
    return lax.broadcasted_iota(jnp.int32, (8, 128), 1)


def rows():
    return lax.broadcasted_iota(jnp.int32, (8, 128), 0)


def roll(v, shift):
    shift %= 128
    return pltpu.roll(v, shift, axis=1) if shift else v


def spot(x, y):
    return (x % 4) * 32 + y


def with_ends(value, ends):
    before = jnp.where(lanes() == 0, ends, roll(value, 1))
    after = jnp.where(lanes() == 127, ends, roll(value, -1))
    return before, after


def clear_if(condition, *outs):
    @pl.when(condition)
    def _():
        for ref in outs:
            ref[...] = jnp.zeros(ref.shape, F32)


def at_first(axis):
    return lax.axis_index(axis) == 0


def at_last(axis):
    return lax.axis_index(axis) == lax.axis_size(axis) - 1


def pack_group(field, g, zp, zm):
    high = jnp.zeros((8, 128), F32)
    low = jnp.zeros((8, 128), F32)
    for xx in range(4):
        for y in range(Y):
            at = spot(xx, y)
            v = roll(field[4 * g + xx, y], at + 1)
            high = jnp.where(lanes() == at, v, high)
            low = jnp.where(lanes() == (at + 1) % 128, v, low)
    zp[g] = high
    zm[g] = low


def pack_columns(field, zp, zm):
    for g in range(4):
        pack_group(field, g, zp, zm)


def start_kernel(rhs, stencil, rc, vi, zp, zm, st, sem_r, sem_s):
    def part(g):
        at = pl.ds(4 * g, 4)
        return pltpu.make_async_copy(rhs.at[:, at], rc.at[:, at], sem_r.at[g])

    def field(k):
        at = WZ_AT[k]
        return pltpu.make_async_copy(stencil.at[k], st.at[at], sem_s.at[at])

    order = [k for pair in PAIRS for k in pair if k is not None]
    for g in range(4):
        part(g).start()
    for k in order:
        field(k).start()

    def group(g, carry):
        part(g).wait()
        for xx in range(4):
            x = 4 * g + xx
            for yb in range(4):
                vi[x, pl.ds(8 * yb, 8)] = jnp.swapaxes(rc[:, x, pl.ds(8 * yb, 8), :], 0, 1)
        pack_group(vi, g, zp, zm)
        return carry

    lax.fori_loop(0, 4, group, 0)
    for k in order:
        field(k).wait()
    for j, (up, down) in enumerate(PAIRS):
        out = jnp.zeros((8, 128), F32)
        for x in range(X):
            for yb in range(4):
                at = 8 * x + 2 * yb
                w = st[WZ_AT[up], x, pl.ds(8 * yb, 8), :]
                if down is not None:
                    w = jnp.where(lanes() == 0, st[WZ_AT[down], x, pl.ds(8 * yb, 8), :], w)
                out = jnp.where((lanes() == at) | (lanes() == at + 1), roll(w, at + 1), out)
        zp[4 + j] = out
        zm[4 + j] = out
    clear_if(at_last("gz"), zp)
    clear_if(at_first("gz"), zm)


def even():
    return (lanes() & 1) == 0


def merged(rl, rr, g):
    left, right = roll(rl[g], 2), rr[g]
    return jnp.where(even(), left, right), jnp.where(even(), right, left)


def ends_of(pair, at):
    return roll(pair[at % 2], -(at + 2))


def coupling_ends(rl, rr):
    return [jnp.where(even(), roll(rl[4 + j], 2), rr[4 + j]) for j in range(5)]


def coupling_end(ends, j, x, yb):
    return roll(ends[j], -(8 * x + 2 * yb + 2))


def roll_rows(vi, vm, vp, x):
    for y in range(Y):
        v = vi[x, y]
        vm[x, y] = roll(v, 1)
        vp[x, y] = roll(v, -1)


def roll_fields(vi, vm, vp):
    def step(n, carry):
        for i in range(8):
            roll_rows(vi, vm, vp, 8 * n + i)
        return carry

    lax.fori_loop(0, X // 8, step, 0)


def roll_kernel(vi, st, vm, vp, wz):
    def step(n, carry):
        for i in range(4):
            x = 4 * n + i
            roll_rows(vi, vm, vp, x)
            for k in ZSHIFTED:
                for yb in range(4):
                    at = pl.ds(8 * yb, 8)
                    wz[WZ_AT[k], x, at, :] = roll(st[k, x, at, :], OFF[k][2])
        return carry

    lax.fori_loop(0, X // 4, step, 0)


def put_ends(rl, rr, vm, vp):
    first, last = lanes() == 0, lanes() == 127

    def groups(n, carry):
        for g in (2 * n, 2 * n + 1):
            pair = merged(rl, rr, g)
            for xx in range(4):
                for y in range(Y):
                    end = ends_of(pair, spot(xx, y))
                    pltpu.store(vm.at[4 * g + xx, y], end, mask=first)
                    pltpu.store(vp.at[4 * g + xx, y], end, mask=last)
        return carry

    lax.fori_loop(0, 2, groups, 0)


def ends_kernel(vm_in, vp_in, wz_in, st, rl, rr, vm, vp, wz, sums):
    put_ends(rl, rr, vm, vp)
    ends = coupling_ends(rl, rr)
    first, last = lanes() == 0, lanes() == 127
    for j, pair in enumerate(PAIRS):
        for x in range(X):
            for yb in range(4):
                end = coupling_end(ends, j, x, yb)
                for k, mask in zip(pair, (first, last)):
                    if k is not None:
                        pltpu.store(wz.at[WZ_AT[k], x, pl.ds(8 * yb, 8), :], end, mask=mask)

    def behind(k, x, yb):
        if k in WZ_AT:
            return wz[WZ_AT[k], x, pl.ds(8 * yb, 8), :]
        return st[k, x, pl.ds(8 * yb, 8), :]

    def add_up(x, carry):
        for yb in range(4):
            total = st[0, x, pl.ds(8 * yb, 8), :]
            for k in OFF:
                total = total + st[k, x, pl.ds(8 * yb, 8), :]
            sums[4, x, pl.ds(8 * yb, 8), :] = total + behind(1, x, yb)
            for i, (a, b) in enumerate(GROUPS):
                keys = [k for k in OFF if OFF[k][:2] == (a, b)]
                sums[i, x, pl.ds(8 * yb, 8), :] = (
                    behind(keys[0], x, yb) + behind(keys[1], x, yb) + behind(keys[2], x, yb)
                )
        return carry

    lax.fori_loop(0, X, add_up, 0)


def ends_again_kernel(vm_in, vp_in, rl, rr, vm, vp):
    put_ends(rl, rr, vm, vp)


def edge_rows(vi, rl, rr, yp, ym):
    for x in range(X):
        yp[x] = vi[x, Y - 1]
        ym[x] = vi[x, 0]
    for g in range(4):
        for i, tile in enumerate(merged(rl, rr, g)):
            yp[16 + 2 * g + i] = tile
            ym[16 + 2 * g + i] = tile


def edge_kernel(vi, st, wz, rl, rr, yp, ym):
    edge_rows(vi, rl, rr, yp, ym)
    ends = coupling_ends(rl, rr)
    for ref, keys, y in ((yp, YPLUS, Y - 1), (ym, YMINUS, 0)):
        rows_of = {}
        for j, pair in enumerate(PAIRS):
            for x in range(X):
                for k, edge in zip(pair, (0, 127)):
                    if k in keys:
                        end = coupling_end(ends, j, x, y // 8)
                        w = wz[WZ_AT[k], x, pl.ds(8 * (y // 8), 8), :]
                        rows_of[k, x] = jnp.where(lanes() == edge, end, w)
        for i, k in enumerate(keys):
            for x in range(X):
                r = 16 * i + x
                if k in WZ_AT:
                    row = rows_of[k, x][y % 8 : y % 8 + 1, :]
                else:
                    row = st[k, x, pl.ds(y, 1), :]
                ref[24 + r // 8, pl.ds(r % 8, 1), :] = row
    clear_if(at_last("gy"), yp)
    clear_if(at_first("gy"), ym)


def edge_again_kernel(vi, rl, rr, yp, ym):
    edge_rows(vi, rl, rr, yp, ym)
    clear_if(at_last("gy"), yp)
    clear_if(at_first("gy"), ym)


def behind_row(st, wz, k, x, y):
    if k in WZ_AT:
        return wz[WZ_AT[k], x, pl.ds(y, 1), :]
    return st[k, x, pl.ds(y, 1), :]


def wide(row):
    return jnp.broadcast_to(row, (8, 128))


def plane(x, first, last, fields, st, wz, acc_ref, at, diag_of):
    cache = {}

    def v(s, dx, y):
        key = (s, dx, y)
        if key not in cache:
            cache[key] = fields[SHIFT_AT[s]][x + dx, y]
        return cache[key]

    coef = {}

    def ahead(k, y):
        if OFF[k][2] == 0:
            if (k, 0, y) not in coef:
                coef[k, 0, y] = wide(st[k, x, pl.ds(y, 1), :])
            return coef[k, 0, y]
        return wide(st[k, x, pl.ds(y, 1), :])

    def behind(k, a, y):
        if k not in WZ_AT:
            if (k, a, y) not in coef:
                coef[k, a, y] = wide(st[k, x - a, pl.ds(y, 1), :])
            return coef[k, a, y]
        return wide(wz[WZ_AT[k], x - a, pl.ds(y, 1), :])

    for y in range(Y):
        parts = [None, None]
        n = 0
        for k, (a, b, c) in OFF.items():
            if 0 <= y + b < Y and not (a == 1 and last):
                term = ahead(k, y) * v(c, a, y + b)
                parts[n % 2] = term if parts[n % 2] is None else parts[n % 2] + term
                n += 1
            if 0 <= y - b < Y and not (a == 1 and first):
                term = behind(k, a, y - b) * v(-c, -a, y - b)
                parts[n % 2] = term if parts[n % 2] is None else parts[n % 2] + term
                n += 1
        acc_ref[at, y] = wide(diag_of(x, y, first)) * v(0, 0, y) - (parts[0] + parts[1])


def interior(fields, st, wz, acc_ref, diag_of):
    plane(0, True, False, fields, st, wz, acc_ref, 0, diag_of)

    def step(x, carry):
        plane(x, False, False, fields, st, wz, acc_ref, x, diag_of)
        return carry

    lax.fori_loop(1, X - 1, step, 0)
    plane(X - 1, False, True, fields, st, wz, acc_ref, X - 1, diag_of)


def inner_kernel(vi, vm, vp, st, wz, sums, acc, diag):
    def diag_of(x, y, first):
        total = sums[4, x, pl.ds(y, 1), :]
        if y > 0:
            total = total + sums[0, x, pl.ds(y - 1, 1), :]
        if not first:
            total = total + sums[2, x - 1, pl.ds(y, 1), :]
            if y > 0:
                total = total + sums[3, x - 1, pl.ds(y - 1, 1), :]
            if y < Y - 1:
                total = total + sums[1, x - 1, pl.ds(y + 1, 1), :]
        diag[x, pl.ds(y, 1), :] = total
        return total

    interior((vi, vm, vp), st, wz, acc, diag_of)


def inner_again_kernel(vi, vm, vp, st, wz, diag, xp, acc, sent):
    sent[...] = xp[...]
    interior((vi, vm, vp), st, wz, acc, lambda x, y, first: diag[x, pl.ds(y, 1), :])


def ring_row(ref, keys, k, x):
    r = 16 * keys.index(k) + x
    return ref[24 + r // 8, pl.ds(r % 8, 1), :]


def third_kernel(with_diag):
    def body(*refs):
        if with_diag:
            vi, vm, vp, st, wz, rl, rr, qm, qp, sums, ring, xm, xp = refs
            qmw, qpw = qm, qp
        else:
            vi, vm, vp, st, wz, rl, rr, qm, qp, qmw, qpw, ring, xm, xp = refs
        for side, q, y in ((0, qm, Y - 1), (1, qp, 0)):
            for x in range(X):
                g = 16 + 2 * (x // 4)
                before, after = with_ends(q[x], ends_of((q[g], q[g + 1]), spot(x, y)))
                ring[side, 0, x] = q[x]
                ring[side, 1, x] = before
                ring[side, 2, x] = after
        xm[0] = qm[0]
        for y in range(Y):
            xm[1 + y] = vi[0, y]
        xm[Y + 1] = qp[0]
        for i, tile in enumerate((*merged(rl, rr, 0), qm[16], qm[17], qp[16], qp[17])):
            xm[Y + 2 + i] = tile
        last = X - 1
        for y in range(Y):
            total = None
            for k in XPLUS:
                _, b, c = OFF[k]
                s = SHIFT_AT[-c]
                if y - b < 0:
                    term = wide(ring_row(qmw, YPLUS, k, last)) * ring[0, s, last]
                elif y - b >= Y:
                    term = wide(ring_row(qpw, YMINUS, k, last)) * ring[1, s, last]
                else:
                    term = wide(behind_row(st, wz, k, last, y - b)) * (vi, vm, vp)[s][last, y - b]
                total = term if total is None else total + term
            xp[y] = total
            if with_diag:
                row = sums[2, last, pl.ds(y, 1), :]
                if y > 0:
                    row = row + sums[3, last, pl.ds(y - 1, 1), :]
                else:
                    for k in (11, 12, 13):
                        row = row + ring_row(qmw, YPLUS, k, last)
                if y < Y - 1:
                    row = row + sums[1, last, pl.ds(y + 1, 1), :]
                else:
                    for k in (5, 6, 7):
                        row = row + ring_row(qpw, YMINUS, k, last)
                xp[Y + y // 8, pl.ds(y % 8, 1), :] = row
        clear_if(at_first("gx"), xm)
        clear_if(at_last("gx"), xp)

    return body


def finish_edges(acc, st, ring, qmw, qpw, tp, tm, extra):
    last = X - 1
    far = {}

    def far_at(s, y):
        if (0, y) not in far:
            base, at = (Y + 2, y) if 0 <= y < Y else ((Y + 4, Y - 1) if y < 0 else (Y + 6, 0))
            far[0, y] = tp[y + 1]
            far[-1, y], far[1, y] = with_ends(tp[y + 1], ends_of((tp[base], tp[base + 1]), at))
        return far[s, y]

    for x in range(X):
        for y in range(Y) if x in (0, last) else (0, Y - 1):
            total = None
            for k, (a, b, c) in OFF.items():
                terms = []
                if x + a == X:
                    terms.append(wide(st[k, x, pl.ds(y, 1), :]) * far_at(c, y + b))
                elif y + b < 0:
                    terms.append(wide(st[k, x, pl.ds(y, 1), :]) * ring[0, SHIFT_AT[c], x + a])
                elif y + b >= Y:
                    terms.append(wide(st[k, x, pl.ds(y, 1), :]) * ring[1, SHIFT_AT[c], x + a])
                if x - a >= 0:
                    if y - b < 0:
                        terms.append(
                            wide(ring_row(qmw, YPLUS, k, x - a)) * ring[0, SHIFT_AT[-c], x - a]
                        )
                    elif y - b >= Y:
                        terms.append(
                            wide(ring_row(qpw, YMINUS, k, x - a)) * ring[1, SHIFT_AT[-c], x - a]
                        )
                for term in terms:
                    total = term if total is None else total + term
            if x == 0 and tm is not None:
                total = tm[y] if total is None else total + tm[y]
            if total is None:
                continue
            value = acc[x, y] - total
            fix = extra(x, y) if extra is not None else None
            acc[x, y] = value if fix is None else value + fix


def join_kernel(acc_in, diag_in, vi, st, ring, qm, qp, tp, tm, acc, diag, zp, zm):
    def fix(x, y):
        row = None
        if y == 0:
            for k in (2, 3, 4):
                r = ring_row(qm, YPLUS, k, x)
                row = r if row is None else row + r
            if x > 0:
                for k in (11, 12, 13):
                    row = row + ring_row(qm, YPLUS, k, x - 1)
        if y == Y - 1 and x > 0:
            for k in (5, 6, 7):
                r = ring_row(qp, YMINUS, k, x - 1)
                row = r if row is None else row + r
        if x == 0:
            r = tm[Y + y // 8, pl.ds(y % 8, 1), :]
            row = r if row is None else row + r
        if row is None:
            return None
        diag[x, pl.ds(y, 1), :] = diag[x, pl.ds(y, 1), :] + row
        return wide(row) * vi[x, y]

    finish_edges(acc, st, ring, qm, qp, tp, tm, fix)
    pack_columns(acc, zp, zm)
    clear_if(at_last("gz"), zp)
    clear_if(at_first("gz"), zm)


def turn_flat(v, out, x):
    for yb in range(4):
        out[:, x, pl.ds(8 * yb, 8), :] = jnp.swapaxes(v[x, pl.ds(8 * yb, 8)], 0, 1)


def flat_kernel(v, out):
    def turn(x, carry):
        turn_flat(v, out, x)
        return carry

    lax.fori_loop(0, X, turn, 0)


PRODUCTS = [(i, j) for i in range(8) for j in range(i, 8)]


def gram(u, v, planes=X, begin=None):
    def step(x, carry):
        for yb in range(4):
            at = pl.ds(8 * yb, 8)
            a = [u[i, x, at, :] for i in range(8)]
            b = a if v is u else [v[i, x, at, :] for i in range(8)]
            carry = tuple(c + a[i] * b[j] for c, (i, j) in zip(carry, PRODUCTS))
        return carry

    if begin is None:
        begin = tuple(jnp.zeros((8, 128), F32) for _ in PRODUCTS)
    return lax.fori_loop(0, planes, step, begin)


def place(tile, sums, m):
    held = dict(zip(PRODUCTS, sums))
    held = {p: jnp.sum(s, axis=1, keepdims=True) for p, s in held.items()}
    for i in range(8):
        row = jnp.zeros((8, 128), F32)
        for j in range(8):
            row = jnp.where(lanes() == 8 * m + j, held[min(i, j), max(i, j)], row)
        row = jnp.broadcast_to(jnp.sum(row, axis=0, keepdims=True), (8, 128))
        mine = (rows() == i) & (lanes() >= 8 * m) & (lanes() < 8 * m + 8)
        tile = jnp.where(mine, row, tile)
    return tile


def gram_first_kernel(r0, out):
    out[...] = place(jnp.zeros((8, 128), F32), gram(r0, r0), 0)


def gram_second_kernel(r0, y1, early, flat, out):
    flat_kernel(y1, flat)
    out[...] = place(early[...], gram(r0, flat), 1)


def gram_third_kernel(y1, early, out):
    out[...] = place(early[...], gram(y1, y1), 2)


def late_kernel(acc_in, st, ring, qm, qp, tp, xp, y1, early, acc, flat, out, far, sent):
    finish_edges(acc, st, ring, qm, qp, tp, None, None)
    for yb in range(4):
        at = pl.ds(8 * yb, 8)
        far[:, 0, at, :] = jnp.swapaxes(tp[pl.ds(8 * yb + 1, 8)], 0, 1)
        sent[:, 0, at, :] = -jnp.swapaxes(xp[at], 0, 1)
    flat_kernel(acc, flat)
    sums = gram(far, sent, 1)
    out[...] = place(early[...], gram(y1, flat, X, sums), 3)


def differences_kernel(r0, y1, y2, tm, d0, d1):
    def step(x, carry):
        for i in range(8):
            d0[i, x] = r0[i, x] - y1[i, x]
            d1[i, x] = y1[i, x] - y2[i, x]
        return carry

    lax.fori_loop(0, X, step, 0)
    for yb in range(4):
        at = pl.ds(8 * yb, 8)
        d1[:, 0, at, :] = d1[:, 0, at, :] + jnp.swapaxes(tm[at], 0, 1)


def entry(col, i):
    return jnp.broadcast_to(col[i : i + 1, :], (8, 128))


def times(left, right):
    result = []
    for j in range(8):
        total = None
        for k in range(8):
            term = left[k] * entry(right[j], k)
            total = term if total is None else total + term
        result.append(total)
    return result


def flip(m):
    result = []
    for j in range(8):
        out = entry(m[0], j)
        for i in range(1, 8):
            out = jnp.where(rows() == i, entry(m[i], j), out)
        result.append(out)
    return result


def plus(left, right):
    return [a + b for a, b in zip(left, right)]


def minus(left, right):
    return [a - b for a, b in zip(left, right)]


def solve(matrix, right):
    a = list(matrix)
    r = list(right)
    for k in range(8):
        inverse = 1.0 / entry(a[k], k)
        here = rows() == k
        for cols, js in ((a, range(k + 1, 8)), (r, range(8))):
            for j in js:
                f = entry(cols[j], k) * inverse
                cols[j] = jnp.where(here, f, cols[j] - a[k] * f)
    return r


def moments(tile, m):
    return [jnp.broadcast_to(tile[:, 8 * m + j : 8 * m + j + 1], (8, 128)) for j in range(8)]


def coefficients(tile):
    m0, m1, m2, m3 = (moments(tile, m) for m in range(4))
    eye = [jnp.where(rows() == j, 1.0, 0.0) for j in range(8)]
    alpha = solve(m1, m0)
    inverse = solve(m0, eye)
    alpha_t = flip(alpha)
    m2a = times(m2, alpha)
    first = times(m1, alpha)
    rr1 = plus(minus(minus(m0, first), flip(first)), times(alpha_t, m2a))
    big = plus(eye, times(inverse, rr1))
    pq = plus(
        times(flip(big), minus(times(m1, big), m2a)),
        times(alpha_t, minus(times(m3, alpha), times(m2, big))),
    )
    alpha2 = solve(pq, rr1)
    return plus(alpha, times(big, alpha2)), times(alpha, alpha2)


def last_kernel(tile_ref, r0, y1, d0, d1, sol, res, coef, sbuf, rbuf, sems):
    c1, c2 = coefficients(tile_ref[...])
    for j in range(8):
        coef[0, j] = c1[j]
        coef[1, j] = c1[j] - c2[j]
        coef[2, j] = c2[j]

    def tile_out(x, yb):
        at = pl.ds(8 * yb, 8)
        a = [d0[i, x, at, :] for i in range(8)]
        b = [y1[i, x, at, :] for i in range(8)]
        c = [d1[i, x, at, :] for i in range(8)]
        for j in range(8):
            sums = []
            for m, field in enumerate((a, b, c)):
                total = None
                for i in range(8):
                    term = wide(coef[m, j, pl.ds(i, 1), :]) * field[i]
                    total = term if total is None else total + term
                sums.append(total)
            sbuf[j, x, at, :] = sums[0] + sums[1]
            rbuf[j, x, at, :] = r0[j, x, at, :] - (sums[1] + sums[2])

    def copy(n, src, dst, which):
        return pltpu.make_async_copy(src.at[:, n], dst.at[:, n], sems.at[which, n])

    def step(n, carry):
        for yb in range(4):
            tile_out(n, yb)
        copy(n, sbuf, sol, 0).start()
        copy(n, rbuf, res, 1).start()
        return carry

    lax.fori_loop(0, X, step, 0)
    for n in range(X):
        copy(n, sbuf, sol, 0).wait()
        copy(n, rbuf, res, 1).wait()


def shift(x, axis, step):
    n = lax.axis_size(axis)
    return lax.ppermute(x, axis, [(i, (i + step) % n) for i in range(n)])


def ring_sum(x, axis, stride):
    left, right, across = (shift(x, axis, n * stride) for n in (1, -1, 2))
    return (x + across) + (left + right)


def other_core(x):
    n = lax.axis_size("gy")
    return lax.ppermute(x, "gy", [(i, i ^ 1) for i in range(n)])


def shards(rhs, stencil):
    full = (X, Y, F, Z)
    compact = (F, X, Y, Z)
    tile = (8, 128)
    dma = pltpu.SemaphoreType.DMA
    st = stencil
    rc, vi, zp, zm = call(
        start_kernel, [rhs, stencil],
        [compact, full, (9, *tile), (9, *tile)],
        in_specs=[FAR] * 2,
        scratch=[pltpu.VMEM((9, X, Y, Z), F32), dma((4,)), dma((9,))],
        limit=START_LIMIT,
    )
    rl = shift(zp, "gz", 1)
    rr = shift(zm, "gz", -1)
    vm, vp, wz = call(roll_kernel, [vi, st], [full, full, (9, X, Y, Z)])
    yp, ym = call(edge_kernel, [vi, st, wz, rl, rr], [(36, *tile), (30, *tile)])
    qm = shift(yp, "gy", 1)
    qp = shift(ym, "gy", -1)
    vm, vp, wz, sums = call(
        ends_kernel, [vm, vp, wz, st, rl, rr],
        [full, full, (9, X, Y, Z), (5, X, Y, Z)], aliases={0: 0, 1: 1, 2: 2}, after=[yp],
    )
    (g0,) = call(gram_first_kernel, [rc], [tile], after=[yp])
    ring, xm, xp = call(
        third_kernel(True), [vi, vm, vp, st, wz, rl, rr, qm, qp, sums],
        [(2, 3, X, *tile), (Y + 8, *tile), (Y + 4, *tile)], after=[g0],
    )
    tp = shift(xm, "gx", -1)
    tm = shift(xp, "gx", 1)
    acc, diag = call(inner_kernel, [vi, vm, vp, st, wz, sums], [full, (X, Y, Z)])
    y1, diag, zp, zm = call(
        join_kernel, [acc, diag, vi, st, ring, qm, qp, tp, tm],
        [full, (X, Y, Z), (4, *tile), (4, *tile)], aliases={0: 0, 1: 1},
    )

    rl = shift(zp, "gz", 1)
    rr = shift(zm, "gz", -1)
    vm, vp = call(roll_fields, [y1], [full, full])
    y1f, g1 = call(gram_second_kernel, [rc, y1, g0], [compact, tile], after=[zp])
    yp, ym = call(edge_again_kernel, [y1, rl, rr], [(24, *tile), (24, *tile)], after=[vm, g1])
    qmv = shift(yp, "gy", 1)
    qpv = shift(ym, "gy", -1)
    vm, vp = call(
        ends_again_kernel, [vm, vp, rl, rr], [full, full],
        aliases={0: 0, 1: 1}, after=[yp],
    )
    (g2,) = call(gram_third_kernel, [y1f, g1], [tile], after=[yp])
    ring, xm, xp = call(
        third_kernel(False), [y1, vm, vp, st, wz, rl, rr, qmv, qpv, qm, qp],
        [(2, 3, X, *tile), (Y + 8, *tile), (Y, *tile)], after=[g2],
    )
    tp = shift(xm, "gx", -1)
    acc, xp = call(inner_again_kernel, [y1, vm, vp, st, wz, diag, xp], [full, (Y, *tile)])
    tm = shift(xp, "gx", 1)
    _, y2f, moment = call(
        late_kernel, [acc, st, ring, qm, qp, tp, xp, y1f, g2],
        [full, compact, tile], aliases={0: 0},
        scratch=[pltpu.VMEM((F, 1, Y, Z), F32), pltpu.VMEM((F, 1, Y, Z), F32)],
    )
    d0, d1 = call(differences_kernel, [rc, y1f, y2f, tm], [compact, compact])
    moment = ring_sum(ring_sum(moment, "gx", 1), "gz", 1)
    moment = ring_sum(moment + other_core(moment), "gy", 2)
    sol, res = call(
        last_kernel, [moment, rc, y1f, d0, d1], [compact, compact],
        out_specs=[FAR, FAR],
        scratch=[
            pltpu.VMEM((3, 8, *tile), F32),
            pltpu.VMEM(compact, F32),
            pltpu.VMEM(compact, F32),
            dma((2, X)),
        ],
        limit=14,
    )
    return sol, res


def solution(mesh):
    placed = P(None, "gx", "gy", "gz")
    return jax.shard_map(
        shards, mesh=mesh, in_specs=(placed, placed), out_specs=(placed, placed), check_vma=False
    )
```

```python
import jax
import jax.numpy as jnp
from jax import lax
from jax.experimental import pallas as pl
from jax.experimental.pallas import tpu as pltpu
from jax.sharding import PartitionSpec as P

F32 = jnp.float32
X, Y, Z, F = 16, 32, 128, 8
FORWARD = [
    (a, b, c) for a in (-1, 0, 1) for b in (-1, 0, 1) for c in (-1, 0, 1) if (a, b, c) > (0, 0, 0)
]
OFF = {k + 1: o for k, o in enumerate(FORWARD)}
ZPLUS = [k for k in OFF if OFF[k][2] == 1]
ZMINUS = [k for k in OFF if OFF[k][2] == -1]
YPLUS = [k for k in OFF if OFF[k][1] == 1]
YMINUS = [k for k in OFF if OFF[k][1] == -1]
XPLUS = [k for k in OFF if OFF[k][0] == 1]
ZSHIFTED = ZPLUS + ZMINUS
WZ_AT = {k: i for i, k in enumerate(ZSHIFTED)}
PAIRS = tuple(zip(ZPLUS, ZMINUS + [None]))
GROUPS = ((0, 1), (1, -1), (1, 0), (1, 1))
SHIFT_AT = {0: 0, -1: 1, 1: 2}

VSPEC = pl.BlockSpec(memory_space=pltpu.VMEM)
HSPEC = pl.BlockSpec(memory_space=pl.ANY)
FAR = pl.BlockSpec(memory_space=pltpu.HBM)
MIB = 1024 * 1024
START_LIMIT = 48


def call(body, ins, outs, after=(), aliases=None, scratch=(), in_specs=None, out_specs=None, limit=8):
    count = len(ins)

    def run(*refs):
        body(*refs[:count], *refs[count + len(after):])

    return pl.pallas_call(
        run,
        out_shape=[jax.ShapeDtypeStruct(s, F32) for s in outs],
        in_specs=(in_specs or [VSPEC] * count) + [HSPEC] * len(after),
        out_specs=out_specs or [VSPEC] * len(outs),
        input_output_aliases=aliases or {},
        scratch_shapes=list(scratch),
        compiler_params=pltpu.CompilerParams(vmem_limit_bytes=limit * MIB),
    )(*ins, *after)


def lanes():
    return lax.broadcasted_iota(jnp.int32, (8, 128), 1)


def rows():
    return lax.broadcasted_iota(jnp.int32, (8, 128), 0)


def roll(v, shift):
    shift %= 128
    return pltpu.roll(v, shift, axis=1) if shift else v


def spot(x, y):
    return (x % 4) * 32 + y


def with_ends(value, ends):
    before = jnp.where(lanes() == 0, ends, roll(value, 1))
    after = jnp.where(lanes() == 127, ends, roll(value, -1))
    return before, after


def clear_if(condition, *outs):
    @pl.when(condition)
    def _():
        for ref in outs:
            ref[...] = jnp.zeros(ref.shape, F32)


def at_first(axis):
    return lax.axis_index(axis) == 0


def at_last(axis):
    return lax.axis_index(axis) == lax.axis_size(axis) - 1


def pack_group(field, g, zp, zm):
    high = jnp.zeros((8, 128), F32)
    low = jnp.zeros((8, 128), F32)
    for xx in range(4):
        for y in range(Y):
            at = spot(xx, y)
            v = roll(field[4 * g + xx, y], at + 1)
            high = jnp.where(lanes() == at, v, high)
            low = jnp.where(lanes() == (at + 1) % 128, v, low)
    zp[g] = high
    zm[g] = low


def pack_columns(field, zp, zm):
    for g in range(4):
        pack_group(field, g, zp, zm)


def start_kernel(rhs, stencil, rc, vi, zp, zm, st, sem_r, sem_s):
    def part(g):
        at = pl.ds(4 * g, 4)
        return pltpu.make_async_copy(rhs.at[:, at], rc.at[:, at], sem_r.at[g])

    def field(k):
        at = WZ_AT[k]
        return pltpu.make_async_copy(stencil.at[k], st.at[at], sem_s.at[at])

    order = [k for pair in PAIRS for k in pair if k is not None]
    for g in range(4):
        part(g).start()
    for k in order:
        field(k).start()

    def group(g, carry):
        part(g).wait()
        for xx in range(4):
            x = 4 * g + xx
            for yb in range(4):
                vi[x, pl.ds(8 * yb, 8)] = jnp.swapaxes(rc[:, x, pl.ds(8 * yb, 8), :], 0, 1)
        pack_group(vi, g, zp, zm)
        return carry

    lax.fori_loop(0, 4, group, 0)
    for k in order:
        field(k).wait()
    for j, (up, down) in enumerate(PAIRS):
        out = jnp.zeros((8, 128), F32)
        for x in range(X):
            for yb in range(4):
                at = 8 * x + 2 * yb
                w = st[WZ_AT[up], x, pl.ds(8 * yb, 8), :]
                if down is not None:
                    w = jnp.where(lanes() == 0, st[WZ_AT[down], x, pl.ds(8 * yb, 8), :], w)
                out = jnp.where((lanes() == at) | (lanes() == at + 1), roll(w, at + 1), out)
        zp[4 + j] = out
        zm[4 + j] = out
    clear_if(at_last("gz"), zp)
    clear_if(at_first("gz"), zm)


def even():
    return (lanes() & 1) == 0


def merged(rl, rr, g):
    left, right = roll(rl[g], 2), rr[g]
    return jnp.where(even(), left, right), jnp.where(even(), right, left)


def ends_of(pair, at):
    return roll(pair[at % 2], -(at + 2))


def coupling_ends(rl, rr):
    return [jnp.where(even(), roll(rl[4 + j], 2), rr[4 + j]) for j in range(5)]


def coupling_end(ends, j, x, yb):
    return roll(ends[j], -(8 * x + 2 * yb + 2))


def roll_rows(vi, vm, vp, x):
    for y in range(Y):
        v = vi[x, y]
        vm[x, y] = roll(v, 1)
        vp[x, y] = roll(v, -1)


def roll_fields(vi, vm, vp):
    def step(n, carry):
        for i in range(8):
            roll_rows(vi, vm, vp, 8 * n + i)
        return carry

    lax.fori_loop(0, X // 8, step, 0)


def roll_kernel(vi, st, vm, vp, wz):
    def step(n, carry):
        for i in range(4):
            x = 4 * n + i
            roll_rows(vi, vm, vp, x)
            for k in ZSHIFTED:
                for yb in range(4):
                    at = pl.ds(8 * yb, 8)
                    wz[WZ_AT[k], x, at, :] = roll(st[k, x, at, :], OFF[k][2])
        return carry

    lax.fori_loop(0, X // 4, step, 0)


def put_ends(rl, rr, vm, vp):
    first, last = lanes() == 0, lanes() == 127

    def groups(n, carry):
        for g in (2 * n, 2 * n + 1):
            pair = merged(rl, rr, g)
            for xx in range(4):
                for y in range(Y):
                    end = ends_of(pair, spot(xx, y))
                    pltpu.store(vm.at[4 * g + xx, y], end, mask=first)
                    pltpu.store(vp.at[4 * g + xx, y], end, mask=last)
        return carry

    lax.fori_loop(0, 2, groups, 0)


def ends_kernel(vm_in, vp_in, wz_in, st, rl, rr, vm, vp, wz, sums):
    put_ends(rl, rr, vm, vp)
    ends = coupling_ends(rl, rr)
    first, last = lanes() == 0, lanes() == 127
    for j, pair in enumerate(PAIRS):
        for x in range(X):
            for yb in range(4):
                end = coupling_end(ends, j, x, yb)
                for k, mask in zip(pair, (first, last)):
                    if k is not None:
                        pltpu.store(wz.at[WZ_AT[k], x, pl.ds(8 * yb, 8), :], end, mask=mask)

    def behind(k, x, yb):
        if k in WZ_AT:
            return wz[WZ_AT[k], x, pl.ds(8 * yb, 8), :]
        return st[k, x, pl.ds(8 * yb, 8), :]

    def add_up(x, carry):
        for yb in range(4):
            total = st[0, x, pl.ds(8 * yb, 8), :]
            for k in OFF:
                total = total + st[k, x, pl.ds(8 * yb, 8), :]
            sums[4, x, pl.ds(8 * yb, 8), :] = total + behind(1, x, yb)
            for i, (a, b) in enumerate(GROUPS):
                keys = [k for k in OFF if OFF[k][:2] == (a, b)]
                sums[i, x, pl.ds(8 * yb, 8), :] = (
                    behind(keys[0], x, yb) + behind(keys[1], x, yb) + behind(keys[2], x, yb)
                )
        return carry

    lax.fori_loop(0, X, add_up, 0)


def ends_again_kernel(vm_in, vp_in, rl, rr, vm, vp):
    put_ends(rl, rr, vm, vp)


def edge_rows(vi, rl, rr, yp, ym):
    for x in range(X):
        yp[x] = vi[x, Y - 1]
        ym[x] = vi[x, 0]
    for g in range(4):
        for i, tile in enumerate(merged(rl, rr, g)):
            yp[16 + 2 * g + i] = tile
            ym[16 + 2 * g + i] = tile


def edge_kernel(vi, st, wz, rl, rr, yp, ym):
    edge_rows(vi, rl, rr, yp, ym)
    ends = coupling_ends(rl, rr)
    for ref, keys, y in ((yp, YPLUS, Y - 1), (ym, YMINUS, 0)):
        rows_of = {}
        for j, pair in enumerate(PAIRS):
            for x in range(X):
                for k, edge in zip(pair, (0, 127)):
                    if k in keys:
                        end = coupling_end(ends, j, x, y // 8)
                        w = wz[WZ_AT[k], x, pl.ds(8 * (y // 8), 8), :]
                        rows_of[k, x] = jnp.where(lanes() == edge, end, w)
        for i, k in enumerate(keys):
            for x in range(X):
                r = 16 * i + x
                if k in WZ_AT:
                    row = rows_of[k, x][y % 8 : y % 8 + 1, :]
                else:
                    row = st[k, x, pl.ds(y, 1), :]
                ref[24 + r // 8, pl.ds(r % 8, 1), :] = row
    clear_if(at_last("gy"), yp)
    clear_if(at_first("gy"), ym)


def edge_again_kernel(vi, rl, rr, yp, ym):
    edge_rows(vi, rl, rr, yp, ym)
    clear_if(at_last("gy"), yp)
    clear_if(at_first("gy"), ym)


def behind_row(st, wz, k, x, y):
    if k in WZ_AT:
        return wz[WZ_AT[k], x, pl.ds(y, 1), :]
    return st[k, x, pl.ds(y, 1), :]


def wide(row):
    return jnp.broadcast_to(row, (8, 128))


def plane(x, first, last, fields, st, wz, acc_ref, at, diag_of):
    cache = {}

    def v(s, dx, y):
        key = (s, dx, y)
        if key not in cache:
            cache[key] = fields[SHIFT_AT[s]][x + dx, y]
        return cache[key]

    coef = {}

    def ahead(k, y):
        if OFF[k][2] == 0:
            if (k, 0, y) not in coef:
                coef[k, 0, y] = wide(st[k, x, pl.ds(y, 1), :])
            return coef[k, 0, y]
        return wide(st[k, x, pl.ds(y, 1), :])

    def behind(k, a, y):
        if k not in WZ_AT:
            if (k, a, y) not in coef:
                coef[k, a, y] = wide(st[k, x - a, pl.ds(y, 1), :])
            return coef[k, a, y]
        return wide(wz[WZ_AT[k], x - a, pl.ds(y, 1), :])

    for y in range(Y):
        parts = [None, None]
        n = 0
        for k, (a, b, c) in OFF.items():
            if 0 <= y + b < Y and not (a == 1 and last):
                term = ahead(k, y) * v(c, a, y + b)
                parts[n % 2] = term if parts[n % 2] is None else parts[n % 2] + term
                n += 1
            if 0 <= y - b < Y and not (a == 1 and first):
                term = behind(k, a, y - b) * v(-c, -a, y - b)
                parts[n % 2] = term if parts[n % 2] is None else parts[n % 2] + term
                n += 1
        acc_ref[at, y] = wide(diag_of(x, y, first)) * v(0, 0, y) - (parts[0] + parts[1])


def interior(fields, st, wz, acc_ref, diag_of):
    plane(0, True, False, fields, st, wz, acc_ref, 0, diag_of)

    def step(x, carry):
        plane(x, False, False, fields, st, wz, acc_ref, x, diag_of)
        return carry

    lax.fori_loop(1, X - 1, step, 0)
    plane(X - 1, False, True, fields, st, wz, acc_ref, X - 1, diag_of)


def inner_kernel(vi, vm, vp, st, wz, sums, acc, diag):
    def diag_of(x, y, first):
        total = sums[4, x, pl.ds(y, 1), :]
        if y > 0:
            total = total + sums[0, x, pl.ds(y - 1, 1), :]
        if not first:
            total = total + sums[2, x - 1, pl.ds(y, 1), :]
            if y > 0:
                total = total + sums[3, x - 1, pl.ds(y - 1, 1), :]
            if y < Y - 1:
                total = total + sums[1, x - 1, pl.ds(y + 1, 1), :]
        diag[x, pl.ds(y, 1), :] = total
        return total

    interior((vi, vm, vp), st, wz, acc, diag_of)


def inner_again_kernel(vi, vm, vp, st, wz, diag, xp, acc, sent):
    sent[...] = xp[...]
    interior((vi, vm, vp), st, wz, acc, lambda x, y, first: diag[x, pl.ds(y, 1), :])


def ring_row(ref, keys, k, x):
    r = 16 * keys.index(k) + x
    return ref[24 + r // 8, pl.ds(r % 8, 1), :]


def third_kernel(with_diag):
    def body(*refs):
        if with_diag:
            vi, vm, vp, st, wz, rl, rr, qm, qp, sums, ring, xm, xp = refs
            qmw, qpw = qm, qp
        else:
            vi, vm, vp, st, wz, rl, rr, qm, qp, qmw, qpw, ring, xm, xp = refs
        for side, q, y in ((0, qm, Y - 1), (1, qp, 0)):
            for x in range(X):
                g = 16 + 2 * (x // 4)
                before, after = with_ends(q[x], ends_of((q[g], q[g + 1]), spot(x, y)))
                ring[side, 0, x] = q[x]
                ring[side, 1, x] = before
                ring[side, 2, x] = after
        xm[0] = qm[0]
        for y in range(Y):
            xm[1 + y] = vi[0, y]
        xm[Y + 1] = qp[0]
        for i, tile in enumerate((*merged(rl, rr, 0), qm[16], qm[17], qp[16], qp[17])):
            xm[Y + 2 + i] = tile
        last = X - 1
        for y in range(Y):
            total = None
            for k in XPLUS:
                _, b, c = OFF[k]
                s = SHIFT_AT[-c]
                if y - b < 0:
                    term = wide(ring_row(qmw, YPLUS, k, last)) * ring[0, s, last]
                elif y - b >= Y:
                    term = wide(ring_row(qpw, YMINUS, k, last)) * ring[1, s, last]
                else:
                    term = wide(behind_row(st, wz, k, last, y - b)) * (vi, vm, vp)[s][last, y - b]
                total = term if total is None else total + term
            xp[y] = total
            if with_diag:
                row = sums[2, last, pl.ds(y, 1), :]
                if y > 0:
                    row = row + sums[3, last, pl.ds(y - 1, 1), :]
                else:
                    for k in (11, 12, 13):
                        row = row + ring_row(qmw, YPLUS, k, last)
                if y < Y - 1:
                    row = row + sums[1, last, pl.ds(y + 1, 1), :]
                else:
                    for k in (5, 6, 7):
                        row = row + ring_row(qpw, YMINUS, k, last)
                xp[Y + y // 8, pl.ds(y % 8, 1), :] = row
        clear_if(at_first("gx"), xm)
        clear_if(at_last("gx"), xp)

    return body


def finish_edges(acc, st, ring, qmw, qpw, tp, tm, extra):
    last = X - 1
    far = {}

    def far_at(s, y):
        if (0, y) not in far:
            base, at = (Y + 2, y) if 0 <= y < Y else ((Y + 4, Y - 1) if y < 0 else (Y + 6, 0))
            far[0, y] = tp[y + 1]
            far[-1, y], far[1, y] = with_ends(tp[y + 1], ends_of((tp[base], tp[base + 1]), at))
        return far[s, y]

    for x in range(X):
        for y in range(Y) if x in (0, last) else (0, Y - 1):
            total = None
            for k, (a, b, c) in OFF.items():
                terms = []
                if x + a == X:
                    terms.append(wide(st[k, x, pl.ds(y, 1), :]) * far_at(c, y + b))
                elif y + b < 0:
                    terms.append(wide(st[k, x, pl.ds(y, 1), :]) * ring[0, SHIFT_AT[c], x + a])
                elif y + b >= Y:
                    terms.append(wide(st[k, x, pl.ds(y, 1), :]) * ring[1, SHIFT_AT[c], x + a])
                if x - a >= 0:
                    if y - b < 0:
                        terms.append(
                            wide(ring_row(qmw, YPLUS, k, x - a)) * ring[0, SHIFT_AT[-c], x - a]
                        )
                    elif y - b >= Y:
                        terms.append(
                            wide(ring_row(qpw, YMINUS, k, x - a)) * ring[1, SHIFT_AT[-c], x - a]
                        )
                for term in terms:
                    total = term if total is None else total + term
            if x == 0 and tm is not None:
                total = tm[y] if total is None else total + tm[y]
            if total is None:
                continue
            value = acc[x, y] - total
            fix = extra(x, y) if extra is not None else None
            acc[x, y] = value if fix is None else value + fix


def join_kernel(acc_in, diag_in, vi, st, ring, qm, qp, tp, tm, acc, diag, zp, zm):
    def fix(x, y):
        row = None
        if y == 0:
            for k in (2, 3, 4):
                r = ring_row(qm, YPLUS, k, x)
                row = r if row is None else row + r
            if x > 0:
                for k in (11, 12, 13):
                    row = row + ring_row(qm, YPLUS, k, x - 1)
        if y == Y - 1 and x > 0:
            for k in (5, 6, 7):
                r = ring_row(qp, YMINUS, k, x - 1)
                row = r if row is None else row + r
        if x == 0:
            r = tm[Y + y // 8, pl.ds(y % 8, 1), :]
            row = r if row is None else row + r
        if row is None:
            return None
        diag[x, pl.ds(y, 1), :] = diag[x, pl.ds(y, 1), :] + row
        return wide(row) * vi[x, y]

    finish_edges(acc, st, ring, qm, qp, tp, tm, fix)
    pack_columns(acc, zp, zm)
    clear_if(at_last("gz"), zp)
    clear_if(at_first("gz"), zm)


def turn_flat(v, out, x):
    for yb in range(4):
        out[:, x, pl.ds(8 * yb, 8), :] = jnp.swapaxes(v[x, pl.ds(8 * yb, 8)], 0, 1)


def flat_kernel(v, out):
    def turn(n, carry):
        for i in range(4):
            turn_flat(v, out, 4 * n + i)
        return carry

    lax.fori_loop(0, X // 4, turn, 0)


PRODUCTS = [(i, j) for i in range(8) for j in range(i, 8)]


def gram(u, v, planes=X, begin=None):
    batch = 2 if planes % 2 == 0 else 1

    def step(n, carry):
        for t in range(4 * batch):
            x, at = batch * n + t // 4, pl.ds(8 * (t % 4), 8)
            a = [u[i, x, at, :] for i in range(8)]
            b = a if v is u else [v[i, x, at, :] for i in range(8)]
            carry = tuple(c + a[i] * b[j] for c, (i, j) in zip(carry, PRODUCTS))
        return carry

    if begin is None:
        begin = tuple(jnp.zeros((8, 128), F32) for _ in PRODUCTS)
    return lax.fori_loop(0, planes // batch, step, begin)


def place(tile, sums, m):
    held = dict(zip(PRODUCTS, sums))
    held = {p: jnp.sum(s, axis=1, keepdims=True) for p, s in held.items()}
    for i in range(8):
        row = jnp.zeros((8, 128), F32)
        for j in range(8):
            row = jnp.where(lanes() == 8 * m + j, held[min(i, j), max(i, j)], row)
        row = jnp.broadcast_to(jnp.sum(row, axis=0, keepdims=True), (8, 128))
        mine = (rows() == i) & (lanes() >= 8 * m) & (lanes() < 8 * m + 8)
        tile = jnp.where(mine, row, tile)
    return tile


def gram_first_kernel(r0, out):
    out[...] = place(jnp.zeros((8, 128), F32), gram(r0, r0), 0)


def gram_second_kernel(r0, y1, early, flat, out):
    flat_kernel(y1, flat)
    out[...] = place(early[...], gram(r0, flat), 1)


def gram_third_kernel(y1, early, out):
    out[...] = place(early[...], gram(y1, y1), 2)


def late_kernel(acc_in, st, ring, qm, qp, tp, xp, y1, early, acc, flat, out, far, sent):
    finish_edges(acc, st, ring, qm, qp, tp, None, None)
    for yb in range(4):
        at = pl.ds(8 * yb, 8)
        far[:, 0, at, :] = jnp.swapaxes(tp[pl.ds(8 * yb + 1, 8)], 0, 1)
        sent[:, 0, at, :] = -jnp.swapaxes(xp[at], 0, 1)
    flat_kernel(acc, flat)
    sums = gram(far, sent, 1)
    out[...] = place(early[...], gram(y1, flat, X, sums), 3)


def differences_kernel(r0, y1, y2, tm, d0, d1):
    def step(x, carry):
        for i in range(8):
            d0[i, x] = r0[i, x] - y1[i, x]
            d1[i, x] = y1[i, x] - y2[i, x]
        return carry

    lax.fori_loop(0, X, step, 0)
    for yb in range(4):
        at = pl.ds(8 * yb, 8)
        d1[:, 0, at, :] = d1[:, 0, at, :] + jnp.swapaxes(tm[at], 0, 1)


def entry(col, i):
    return jnp.broadcast_to(col[i : i + 1, :], (8, 128))


def times(left, right):
    result = []
    for j in range(8):
        total = None
        for k in range(8):
            term = left[k] * entry(right[j], k)
            total = term if total is None else total + term
        result.append(total)
    return result


def flip(m):
    result = []
    for j in range(8):
        out = entry(m[0], j)
        for i in range(1, 8):
            out = jnp.where(rows() == i, entry(m[i], j), out)
        result.append(out)
    return result


def plus(left, right):
    return [a + b for a, b in zip(left, right)]


def minus(left, right):
    return [a - b for a, b in zip(left, right)]


def solve(matrix, right):
    a = list(matrix)
    r = list(right)
    for k in range(8):
        inverse = 1.0 / entry(a[k], k)
        here = rows() == k
        for cols, js in ((a, range(k + 1, 8)), (r, range(8))):
            for j in js:
                f = entry(cols[j], k) * inverse
                cols[j] = jnp.where(here, f, cols[j] - a[k] * f)
    return r


def moments(tile, m):
    return [jnp.broadcast_to(tile[:, 8 * m + j : 8 * m + j + 1], (8, 128)) for j in range(8)]


def coefficients(tile):
    m0, m1, m2, m3 = (moments(tile, m) for m in range(4))
    eye = [jnp.where(rows() == j, 1.0, 0.0) for j in range(8)]
    alpha = solve(m1, m0)
    inverse = solve(m0, eye)
    alpha_t = flip(alpha)
    m2a = times(m2, alpha)
    first = times(m1, alpha)
    rr1 = plus(minus(minus(m0, first), flip(first)), times(alpha_t, m2a))
    big = plus(eye, times(inverse, rr1))
    pq = plus(
        times(flip(big), minus(times(m1, big), m2a)),
        times(alpha_t, minus(times(m3, alpha), times(m2, big))),
    )
    alpha2 = solve(pq, rr1)
    return plus(alpha, times(big, alpha2)), times(alpha, alpha2)


def last_kernel(tile_ref, r0, y1, d0, d1, sol, res, coef, sbuf, rbuf, sems):
    c1, c2 = coefficients(tile_ref[...])
    for j in range(8):
        coef[0, j] = c1[j]
        coef[1, j] = c1[j] - c2[j]
        coef[2, j] = c2[j]

    def tile_out(x, yb):
        at = pl.ds(8 * yb, 8)
        a = [d0[i, x, at, :] for i in range(8)]
        b = [y1[i, x, at, :] for i in range(8)]
        c = [d1[i, x, at, :] for i in range(8)]
        for j in range(8):
            sums = []
            for m, field in enumerate((a, b, c)):
                total = None
                for i in range(8):
                    term = wide(coef[m, j, pl.ds(i, 1), :]) * field[i]
                    total = term if total is None else total + term
                sums.append(total)
            sbuf[j, x, at, :] = sums[0] + sums[1]
            rbuf[j, x, at, :] = r0[j, x, at, :] - (sums[1] + sums[2])

    def copy(n, src, dst, which):
        return pltpu.make_async_copy(src.at[:, n], dst.at[:, n], sems.at[which, n])

    def step(n, carry):
        for yb in range(4):
            tile_out(n, yb)
        copy(n, sbuf, sol, 0).start()
        copy(n, rbuf, res, 1).start()
        return carry

    lax.fori_loop(0, X, step, 0)
    for n in range(X):
        copy(n, sbuf, sol, 0).wait()
        copy(n, rbuf, res, 1).wait()


def shift(x, axis, step):
    n = lax.axis_size(axis)
    return lax.ppermute(x, axis, [(i, (i + step) % n) for i in range(n)])


def ring_sum(x, axis, stride):
    left, right, across = (shift(x, axis, n * stride) for n in (1, -1, 2))
    return (x + across) + (left + right)


def other_core(x):
    n = lax.axis_size("gy")
    return lax.ppermute(x, "gy", [(i, i ^ 1) for i in range(n)])


def shards(rhs, stencil):
    full = (X, Y, F, Z)
    compact = (F, X, Y, Z)
    tile = (8, 128)
    dma = pltpu.SemaphoreType.DMA
    st = stencil
    rc, vi, zp, zm = call(
        start_kernel, [rhs, stencil],
        [compact, full, (9, *tile), (9, *tile)],
        in_specs=[FAR] * 2,
        scratch=[pltpu.VMEM((9, X, Y, Z), F32), dma((4,)), dma((9,))],
        limit=START_LIMIT,
    )
    rl = shift(zp, "gz", 1)
    rr = shift(zm, "gz", -1)
    vm, vp, wz = call(roll_kernel, [vi, st], [full, full, (9, X, Y, Z)])
    yp, ym = call(edge_kernel, [vi, st, wz, rl, rr], [(36, *tile), (30, *tile)])
    qm = shift(yp, "gy", 1)
    qp = shift(ym, "gy", -1)
    vm, vp, wz, sums = call(
        ends_kernel, [vm, vp, wz, st, rl, rr],
        [full, full, (9, X, Y, Z), (5, X, Y, Z)], aliases={0: 0, 1: 1, 2: 2}, after=[yp],
    )
    (g0,) = call(gram_first_kernel, [rc], [tile], after=[yp])
    ring, xm, xp = call(
        third_kernel(True), [vi, vm, vp, st, wz, rl, rr, qm, qp, sums],
        [(2, 3, X, *tile), (Y + 8, *tile), (Y + 4, *tile)], after=[g0],
    )
    tp = shift(xm, "gx", -1)
    tm = shift(xp, "gx", 1)
    acc, diag = call(inner_kernel, [vi, vm, vp, st, wz, sums], [full, (X, Y, Z)])
    y1, diag, zp, zm = call(
        join_kernel, [acc, diag, vi, st, ring, qm, qp, tp, tm],
        [full, (X, Y, Z), (4, *tile), (4, *tile)], aliases={0: 0, 1: 1},
    )

    rl = shift(zp, "gz", 1)
    rr = shift(zm, "gz", -1)
    vm, vp = call(roll_fields, [y1], [full, full])
    y1f, g1 = call(gram_second_kernel, [rc, y1, g0], [compact, tile], after=[zp])
    yp, ym = call(edge_again_kernel, [y1, rl, rr], [(24, *tile), (24, *tile)], after=[vm, g1])
    qmv = shift(yp, "gy", 1)
    qpv = shift(ym, "gy", -1)
    vm, vp = call(
        ends_again_kernel, [vm, vp, rl, rr], [full, full],
        aliases={0: 0, 1: 1}, after=[yp],
    )
    (g2,) = call(gram_third_kernel, [y1f, g1], [tile], after=[yp])
    ring, xm, xp = call(
        third_kernel(False), [y1, vm, vp, st, wz, rl, rr, qmv, qpv, qm, qp],
        [(2, 3, X, *tile), (Y + 8, *tile), (Y, *tile)], after=[g2],
    )
    tp = shift(xm, "gx", -1)
    acc, xp = call(inner_again_kernel, [y1, vm, vp, st, wz, diag, xp], [full, (Y, *tile)])
    tm = shift(xp, "gx", 1)
    _, y2f, moment = call(
        late_kernel, [acc, st, ring, qm, qp, tp, xp, y1f, g2],
        [full, compact, tile], aliases={0: 0},
        scratch=[pltpu.VMEM((F, 1, Y, Z), F32), pltpu.VMEM((F, 1, Y, Z), F32)],
    )
    d0, d1 = call(differences_kernel, [rc, y1f, y2f, tm], [compact, compact])
    moment = ring_sum(ring_sum(moment, "gx", 1), "gz", 1)
    moment = ring_sum(moment + other_core(moment), "gy", 2)
    sol, res = call(
        last_kernel, [moment, rc, y1f, d0, d1], [compact, compact],
        out_specs=[FAR, FAR],
        scratch=[
            pltpu.VMEM((3, 8, *tile), F32),
            pltpu.VMEM(compact, F32),
            pltpu.VMEM(compact, F32),
            dma((2, X)),
        ],
        limit=14,
    )
    return sol, res


def solution(mesh):
    placed = P(None, "gx", "gy", "gz")
    return jax.shard_map(
        shards, mesh=mesh, in_specs=(placed, placed), out_specs=(placed, placed), check_vma=False
    )
```
